512 devices in a mesh: seq: 8 (over z), mp: 16 (over y, core), dp: 4 (over x).
Axes of the slice: x: 4, y: 8, z: 8, core: 2. Of those that a mesh axis runs over, the one named last changes fastest.
Arguments:
- tokens: bfloat16 [65536, 2048], P(('dp', 'seq'), 'mp'), parts along dimension 0, may hold values from -6 to 6
- w_query: bfloat16 [2048, 2048], P(None, 'mp'), may hold values from -0.125 to 0.125
- w_key: bfloat16 [2048, 2048], P(None, 'mp'), may hold values from -0.125 to 0.125
- w_value: bfloat16 [2048, 2048], P(None, 'mp'), may hold values from -0.125 to 0.125
- w_gate: bfloat16 [2048, 2048], P(None, 'mp'), may hold values from -0.125 to 0.125
- decay_exponent: int32 [16], P('mp'), may hold values from 5 to 16
- forget: float32 [65536, 16], P(('dp', 'seq'), 'mp'), parts along dimension 0, may hold values from 0 to 0.69
- norm_gain: float32 [2048], replicated, may hold values from 0.1 to 1.9
Outputs:
- retained: bfloat16 [65536, 2048], P(('dp', 'seq', 'mp')), parts along dimension 0
The draws below stay inside these ranges and needn't reach their ends.
There are 4 independent parts, one for each index of `dp`. The reference program is written for one: setup_inputs(seed, part) draws one part's arguments, and reference() takes and returns one part's arrays. A program takes and returns all parts, laid end to end along the dimension named above; an argument that names none is the same for every part. Nothing has to cross between parts.
All inputs are finite; a program needn't handle non-finite values.
Results may differ from the reference program's by a relative error of at most 0.015.
Values may be sent and summed in bfloat16 or wider, within the bound.
A program may use at most 64 MiB of HBM per device.

```python
import jax
import jax.numpy as jnp
from jax import lax

D = 2048
HEADS = 16
DH = 128
TOKENS = 16384
FEATURES = 2048


def draw_forget(key, part):
    first_key, second_key = jax.random.split(jax.random.fold_in(key, 11))
    chance = jax.random.uniform(first_key, (TOKENS, HEADS), jnp.float32)
    amount = jax.random.uniform(second_key, (TOKENS, HEADS), jnp.float32, 0.22, 0.69)
    return jnp.where(chance < 6.0 / TOKENS, amount, 0.0).astype(jnp.float32)


def with_ends(entries, key, low, high):
    spot = [jax.random.randint(jax.random.fold_in(key, axis), (), 0, length) for axis, length in enumerate(entries.shape)]
    longest = entries.shape.index(max(entries.shape))
    next_to = spot[:longest] + [(spot[longest] + 1) % entries.shape[longest]] + spot[longest + 1:]
    return entries.at[tuple(spot)].set(low).at[tuple(next_to)].set(high)


def level_of(rng, extent, shards, smallest, top_value):
    level, own = 1.0, jax.random.fold_in(rng, 6)
    for axis_at, shards_of in shards:
        heights = jnp.exp(jax.random.uniform(jax.random.fold_in(own, axis_at), (shards_of,), jnp.float32, smallest / len(shards), top_value / len(shards)))
        level = level * jnp.repeat(heights, extent[axis_at] // shards_of).reshape([-1 if axis == axis_at else 1 for axis in range(len(extent))])
    return level


def normal_values(key, extent, spread, reach, shards=(), kind=jnp.bfloat16):
    level = level_of(key, extent, shards, -0.22, 0.18) if shards else 1.0
    values = jax.random.normal(key, extent, jnp.float32) * spread * level
    return jnp.minimum(jnp.maximum(values, -reach), reach).astype(kind)


def setup_inputs(seed: int = 0, part: int = 0) -> dict:
    keys = jax.random.split(jax.random.key(seed), 9)
    part_splits = jax.random.split(jax.random.fold_in(keys[8], part), 9)
    return {
        "tokens": normal_values(part_splits[0], (TOKENS, D), 1.0, 6.0, ((0, 8), (1, 16))),
        "w_query": normal_values(keys[1], (D, FEATURES), D ** -0.5, 0.125, ((1, 16),)),
        "w_key": normal_values(keys[2], (D, FEATURES), D ** -0.5, 0.125, ((1, 16),)),
        "w_value": normal_values(keys[3], (D, FEATURES), D ** -0.5, 0.125, ((1, 16),)),
        "w_gate": normal_values(keys[4], (D, FEATURES), D ** -0.5, 0.125, ((1, 16),)),
        "decay_exponent": with_ends(jax.random.randint(keys[5], (HEADS,), 5, 17), jax.random.fold_in(keys[5], 1), 5, 16).astype(jnp.int32),
        "forget": draw_forget(jax.random.fold_in(jax.random.fold_in(keys[8], part), 71), part),
        "norm_gain": jnp.clip(1.0 + 0.18 * jax.random.normal(keys[7], (FEATURES,), jnp.float32), 0.1, 1.9),
    }


def retention(queries, key_rows, values, logdecay):
    seq_rows = queries.shape[0]
    head_count = logdecay.shape[1]
    head_width = queries.shape[1] // head_count
    block_rows = 512 if seq_rows % 512 == 0 else seq_rows
    block_count = seq_rows // block_rows

    def shaped(source):
        return source.reshape(block_count, block_rows, head_count, head_width)
    decays = logdecay.reshape(block_count, block_rows, head_count)
    position = lax.broadcasted_iota(jnp.int32, (block_rows, block_rows), 0)
    earlier = lax.broadcasted_iota(jnp.int32, (block_rows, block_rows), 1)
    causal = position >= earlier

    def advance(kv_state, pieces):
        query_blk, key_blk, value_blk, decay_blk = pieces
        running = jnp.cumsum(decay_blk, axis=0)
        heads_first = running.T
        log_gap = heads_first[:, :, None] - heads_first[:, None, :]
        decay_mask = jnp.where(causal[None], jnp.exp(jnp.where(causal[None], log_gap, 0.0)), 0.0)
        query_float = query_blk.astype(jnp.float32)
        key_float = key_blk.astype(jnp.float32)
        value_float = value_blk.astype(jnp.float32)
        scores = (jnp.einsum('tha,sha->hts', query_float, key_float) * decay_mask).astype(jnp.bfloat16)
        inner = jnp.einsum('hts,shb->thb', scores.astype(jnp.float32), value_float)
        carried = jnp.einsum('tha,hab->thb', query_float * jnp.exp(running)[:, :, None], kv_state, precision=lax.Precision.HIGHEST)
        key_scaled = key_float * jnp.exp(running[-1:] - running)[:, :, None]
        kv_state = jnp.exp(running[-1])[:, None, None] * kv_state + jnp.einsum('sha,shb->hab', key_scaled, value_float, precision=lax.Precision.HIGHEST)
        return (kv_state, (inner + carried).astype(jnp.bfloat16))
    initial = jnp.zeros((head_count, head_width, head_width), jnp.float32)
    final_state, outputs = lax.scan(advance, initial, (shaped(queries), shaped(key_rows), shaped(values), decays))
    return outputs.reshape(seq_rows, head_count * head_width)

def reference(tokens, w_query, w_key, w_value, w_gate, decay_exponent, forget, norm_gain):
    queries = jnp.dot(tokens, w_query, preferred_element_type=jnp.float32).astype(jnp.bfloat16)
    key_rows = (jnp.dot(tokens, w_key, preferred_element_type=jnp.float32) * DH ** (-0.5)).astype(jnp.bfloat16)
    values = jnp.dot(tokens, w_value, preferred_element_type=jnp.float32).astype(jnp.bfloat16)
    gate = jnp.dot(tokens, w_gate, preferred_element_type=jnp.float32).astype(jnp.bfloat16)
    rate = jnp.log1p(-jnp.exp2(-decay_exponent.astype(jnp.float32)))
    logdecay = rate[None, :] - forget
    output = retention(queries, key_rows, values, logdecay).astype(jnp.float32)
    squares = lax.optimization_barrier(jnp.mean(output * output, axis=1))
    rstd = lax.rsqrt(squares + 1e-06)
    gated = jax.nn.silu(gate.astype(jnp.float32)) * output * rstd[:, None] * norm_gain[None, :]
    return gated.astype(jnp.bfloat16)
```

```python
import jax
import jax.numpy as jnp
from jax import lax
from jax.experimental import pallas as pl
from jax.experimental.pallas import tpu as pltpu
from jax.sharding import PartitionSpec as P

DH = 128
CHIPS = 8
BLOCK = 256
BLOCKS = 8
GROUP = 4
MESH = pl.DeviceIdType.MESH
F32 = jnp.float32
BF16 = jnp.bfloat16
PLACE = {0: 0, 1: 1, 7: 2, 2: 3, 6: 4, 3: 5, 5: 6, 4: 7}
ORDER = [0, 1, 7, 2, 6, 3, 5, 4]


def ring_lists():
    right, left = [], []
    for base in range(0, BLOCKS, GROUP):
        even = [base, base + 2, base + 1, base + 3]
        odd = [base + 1, base + 3, base, base + 2]
        for d in (1, 2, 3):
            right += [(j, d) for j in even]
            left += [(j, d) for j in odd]
        right += [(j, 4) for j in even[:2]]
        left += [(j, 4) for j in odd[:2]]
    return right, left


RIGHT, LEFT = ring_lists()
SENDS = len(RIGHT)


def dot(a, b):
    return jnp.dot(a, b, preferred_element_type=F32)


def dot_t(a, b):
    return lax.dot_general(a, b, (((1,), (1,)), ((), ())), preferred_element_type=F32)


def t_dot(a, b):
    return lax.dot_general(a, b, (((0,), (0,)), ((), ())), preferred_element_type=F32)


def kernel(
    tok_hbm, wq_hbm, wk_hbm, wv_hbm, wg_hbm, logd_ref, gain_ref, out_ref,
    tok, w, decay, kdec, qdec, ends, sg, qd, vb, kb, olocal, states, start, own_state, own_total,
    got_state, got_total, ubuf, ssbuf, obuf, ssgot, carried,
    tok_sem, w_sem, right_sem, left_sem, pair_sem, sent_right, sent_left, sent_pair,
    state_sem, total_sem, state_sent, total_sent, o_sem, ss_sem, o_sent, ss_sent, self_sem,
):
    m = lax.axis_index("mp")
    z = lax.axis_index("seq")
    core = lax.rem(m, 2)
    y = m // 2
    pair = m + 1 - 2 * core
    to_right = lax.rem(m + 2, 16)
    to_left = lax.rem(m + 14, 16)

    barrier = pltpu.get_barrier_semaphore()
    for e in range(1, 16):
        pl.semaphore_signal(barrier, inc=1, device_id={"mp": lax.rem(m + e, 16)}, device_id_type=MESH)
    for e in range(1, 8):
        pl.semaphore_signal(barrier, inc=1, device_id={"seq": lax.rem(z + e, 8)}, device_id_type=MESH)

    def columns(place, of):
        return pl.ds(pl.multiple_of(place * 256 + of * 128, 128), 128)

    own_copy = pltpu.make_async_copy(tok_hbm, tok.at[:, columns(0, core)], tok_sem)
    own_copy.start()
    for r in ORDER:
        source = pl.ds(pl.multiple_of(lax.rem(y + 8 - r, 8) * 256, 256), 256)
        rows = pl.ds(PLACE[r] * 256, 256)
        for n, weight in enumerate((wk_hbm, wv_hbm, wq_hbm, wg_hbm)):
            pltpu.make_async_copy(weight.at[source], w.at[rows, pl.ds(n * 128, 128)], w_sem).start()

    logd = logd_ref[...]
    lane = lax.broadcasted_iota(jnp.int32, (16, 128), 1)
    row = lax.broadcasted_iota(jnp.int32, (16, 128), 0)
    run = logd
    for shift in (1, 2, 4, 8, 16, 32, 64):
        run = run + jnp.where(lane >= shift, pltpu.roll(run, shift, 1), 0.0)
    half_sum = jnp.broadcast_to(run[:, 127:128], (16, 128))
    run = run + jnp.where(row % 2 == 1, pltpu.roll(half_sum, 1, 0), 0.0)
    turned = run.T
    before = jnp.zeros((8, 128), F32)
    for j in range(BLOCKS):
        end = jnp.broadcast_to(run[2 * j + 1 : 2 * j + 2, 127:128], (8, 128))
        ends[0, j] = end
        ends[1, j] = before
        before = before + end
    own_total[...] = before

    pl.semaphore_wait(barrier, 22)
    own_copy.wait()

    def ring_copy(direction, index):
        j, d = (RIGHT if direction > 0 else LEFT)[index]
        source = (d - 1) if direction > 0 else (8 - (d - 1)) % 8
        target = d if direction > 0 else 8 - d
        rows = pl.ds(j * BLOCK, BLOCK)
        return pltpu.make_async_remote_copy(
            src_ref=tok.at[rows, columns(PLACE[source], core)],
            dst_ref=tok.at[rows, columns(PLACE[target], core)],
            send_sem=sent_right if direction > 0 else sent_left,
            recv_sem=(right_sem if direction > 0 else left_sem).at[index],
            device_id={"mp": to_right if direction > 0 else to_left},
            device_id_type=MESH,
        )

    def pair_copy(j, r):
        rows = pl.ds(j * BLOCK, BLOCK)
        spot = tok.at[rows, columns(PLACE[r], core)]
        return pltpu.make_async_remote_copy(
            src_ref=spot, dst_ref=spot, send_sem=sent_pair, recv_sem=pair_sem.at[j],
            device_id={"mp": pair}, device_id_type=MESH,
        )

    for index in range(GROUP):
        ring_copy(1, index).start()
        ring_copy(-1, index).start()
    for j in range(BLOCKS):
        pair_copy(j, 0).start()

    def total_copy(e):
        return pltpu.make_async_remote_copy(
            src_ref=own_total, dst_ref=got_total.at[e - 1], send_sem=total_sent.at[e - 1],
            recv_sem=total_sem.at[e - 1], device_id={"seq": lax.rem(z + e, 8)}, device_id_type=MESH,
        )

    def state_copy(e):
        return pltpu.make_async_remote_copy(
            src_ref=own_state, dst_ref=got_state.at[e - 1], send_sem=state_sent.at[e - 1],
            recv_sem=state_sem.at[e - 1], device_id={"seq": lax.rem(z + e, 8)}, device_id_type=MESH,
        )

    for e in range(1, 8):

        @pl.when(z + e < 8)
        def _():
            total_copy(e).start()

    def make_decay(j):
        rows = pl.ds(j * BLOCK, BLOCK)
        down = jnp.concatenate([turned[:, 2 * j : 2 * j + 1], turned[:, 2 * j + 1 : 2 * j + 2]], axis=0)
        across = jnp.concatenate([run[2 * j : 2 * j + 1], run[2 * j + 1 : 2 * j + 2]], axis=1)
        t = lax.broadcasted_iota(jnp.int32, (BLOCK, BLOCK), 0)
        s = lax.broadcasted_iota(jnp.int32, (BLOCK, BLOCK), 1)
        gap = jnp.where(t >= s, down - across, 0.0)
        decay[j] = jnp.where(t >= s, jnp.exp(gap), 0.0)
        wide = jnp.broadcast_to(down, (BLOCK, DH))
        qdec[rows] = jnp.exp(wide)
        kdec[rows] = jnp.exp(ends[0, j, 0:1] - wide)

    def project_kv(j):
        rows = pl.ds(pl.multiple_of(j * BLOCK, BLOCK), BLOCK)
        both = dot(tok[rows], w[:, 0:256])
        keys = (both[:, :128] * DH**-0.5).astype(BF16)
        values = both[:, 128:].astype(BF16)
        kb[rows] = keys
        vb[rows] = values
        faded = (keys.astype(F32) * kdec[rows]).astype(BF16)
        start[j] = carried[...]
        carried[...] = jnp.exp(ends[0, j, 0:1]) * carried[...] + t_dot(faded, values)

    def project_qg(j):
        rows = pl.ds(pl.multiple_of(j * BLOCK, BLOCK), BLOCK)
        both = dot(tok[rows], w[:, 256:512])
        queries = both[:, :128].astype(BF16)
        gate = both[:, 128:].astype(BF16).astype(F32)
        sg[rows] = gate / (1.0 + jnp.exp(-gate)) * gain_ref[pl.ds(m, 1), :]
        qd[rows] = (queries.astype(F32) * qdec[rows]).astype(BF16)
        scores = (dot_t(queries, kb[rows]) * decay[j]).astype(BF16)
        olocal[rows] = dot(scores, vb[rows])

    def wait_weights():
        pltpu.make_async_copy(w, w, w_sem).wait()

    carried[...] = jnp.zeros_like(carried)
    ready = 14
    for index in range(SENDS):
        for direction in (1, -1):
            ring_copy(direction, index).wait_recv()
            if index + GROUP < SENDS:
                ring_copy(direction, index + GROUP).start()
            j, d = (RIGHT if direction > 0 else LEFT)[index]
            pair_copy(j, d if direction > 0 else 8 - d).start()
        if index < BLOCKS:
            make_decay(index)
        if index == ready:
            wait_weights()
            for j in range(GROUP):
                pltpu.make_async_copy(tok.at[pl.ds(0, BLOCK), pl.ds(0, 1024)], tok.at[pl.ds(0, BLOCK), pl.ds(0, 1024)], pair_sem.at[j]).wait()
        piece = index - ready - 1
        if 0 <= piece < 2 * GROUP:
            (project_qg if piece % 2 else project_kv)(piece // 2)

    for j in range(GROUP, BLOCKS):
        pltpu.make_async_copy(tok.at[pl.ds(0, BLOCK), pl.ds(0, 1024)], tok.at[pl.ds(0, BLOCK), pl.ds(0, 1024)], pair_sem.at[j]).wait()

    def each(lower, upper, run_one):
        def step(j, _):
            run_one(j)
            return 0

        lax.fori_loop(lower, upper, step, 0)

    each(GROUP, BLOCKS, project_kv)
    own_state[...] = carried[...].astype(BF16)
    for e in range(1, 8):

        @pl.when(z + e < 8)
        def _():
            state_copy(e).start()

    each(GROUP, BLOCKS, project_qg)

    carried[...] = jnp.zeros_like(carried)
    states[...] = jnp.zeros_like(states)
    for e in range(1, 8):

        @pl.when(z >= e)
        def _():
            total_copy(e).wait_recv()
            state_copy(e).wait_recv()
            carried[...] += jnp.exp(states[0:1]) * got_state[e - 1].astype(F32)
            states[...] += got_total[e - 1]

    one = jnp.ones((8, 128), BF16)

    def out_copy(j, other, r):
        target = 2 * j + other
        return (
            pltpu.make_async_remote_copy(
                src_ref=ubuf.at[j, pl.ds(pl.multiple_of(other * 128, 128), 128)], dst_ref=obuf.at[m], send_sem=o_sent, recv_sem=o_sem,
                device_id={"mp": target}, device_id_type=MESH,
            ),
            pltpu.make_async_remote_copy(
                src_ref=ssbuf.at[j, other], dst_ref=ssgot.at[m], send_sem=ss_sent, recv_sem=ss_sem,
                device_id={"mp": target}, device_id_type=MESH,
            ),
        )

    for r in (4, 3, 5, 2, 6, 1, 7, 0):
        j = lax.rem(y + r, 8)
        rows = pl.ds(pl.multiple_of(j * BLOCK, BLOCK), BLOCK)
        entering = start[j] + jnp.exp(ends[1, j, 0:1]) * carried[...]
        o = (olocal[rows] + dot(qd[rows], entering.astype(BF16))).astype(BF16).astype(F32)
        ubuf[j] = (sg[rows] * o).astype(BF16)
        square = o * o
        high = square.astype(BF16)
        low = (square - high.astype(F32)).astype(BF16)
        total = dot_t(one, high) + dot_t(one, low)
        ssbuf[j, 0] = total[:, :128]
        ssbuf[j, 1] = total[:, 128:]
        if r:
            for other in (0, 1):
                for copy in out_copy(j, other, r):
                    copy.start()
        else:
            for copy in out_copy(j, 1 - core, r):
                copy.start()
            mine = pl.ds(pl.multiple_of(core * 128, 128), 128)
            keep = (
                pltpu.make_async_copy(ubuf.at[j, mine], obuf.at[m], self_sem.at[0]),
                pltpu.make_async_copy(ssbuf.at[j, core], ssgot.at[m], self_sem.at[1]),
            )
            for copy in keep:
                copy.start()
            for copy in keep:
                copy.wait()

    pltpu.make_async_copy(ssgot.at[pl.ds(0, 15)], ssgot.at[pl.ds(0, 15)], ss_sem).wait()
    pltpu.make_async_copy(obuf.at[pl.ds(0, 15)], obuf.at[pl.ds(0, 15)], o_sem).wait()
    squares = ssgot[0]
    for n in range(1, 16):
        squares = squares + ssgot[n]
    rstd = lax.rsqrt(squares / 2048.0 + 1e-06)
    down = jnp.broadcast_to(rstd[0:1], (128, 128)).T
    for n in range(16):
        out_ref[:, n * 128 : (n + 1) * 128] = (obuf[n].astype(F32) * down).astype(BF16)

    for sem in (sent_right, sent_left):
        spot = tok.at[pl.ds(0, SENDS * 16), :]
        pltpu.make_async_copy(spot, spot, sem).wait()
    spot = tok.at[:, pl.ds(0, 1024)]
    pltpu.make_async_copy(spot, spot, sent_pair).wait()
    pltpu.make_async_copy(obuf.at[pl.ds(0, 15)], obuf.at[pl.ds(0, 15)], o_sent).wait()
    pltpu.make_async_copy(ssgot.at[pl.ds(0, 15)], ssgot.at[pl.ds(0, 15)], ss_sent).wait()
    for e in range(1, 8):

        @pl.when(z + e < 8)
        def _():
            total_copy(e).wait_send()
            state_copy(e).wait_send()


def body(tokens, w_query, w_key, w_value, w_gate, decay_exponent, forget, norm_gain):
    rate = jnp.log1p(-jnp.exp2(-decay_exponent.astype(F32)))
    logd = rate[0] - forget.reshape(16, 128)
    gain = norm_gain.reshape(16, 128)
    vmem = pl.BlockSpec(memory_space=pltpu.VMEM)
    anywhere = pl.BlockSpec(memory_space=pl.ANY)
    dma = pltpu.SemaphoreType.DMA
    return pl.pallas_call(
        kernel,
        out_shape=jax.ShapeDtypeStruct((128, 2048), BF16),
        in_specs=[anywhere] * 5 + [vmem] * 2,
        out_specs=vmem,
        scratch_shapes=[
            pltpu.VMEM((2048, 2048), BF16),
            pltpu.VMEM((2048, 512), BF16),
            pltpu.VMEM((8, BLOCK, BLOCK), F32),
            pltpu.VMEM((2048, 128), F32),
            pltpu.VMEM((2048, 128), F32),
            pltpu.VMEM((2, 8, 8, 128), F32),
            pltpu.VMEM((2048, 128), F32),
            pltpu.VMEM((2048, 128), BF16),
            pltpu.VMEM((2048, 128), BF16),
            pltpu.VMEM((2048, 128), BF16),
            pltpu.VMEM((2048, 128), F32),
            pltpu.VMEM((8, 128), F32),
            pltpu.VMEM((8, 128, 128), F32),
            pltpu.VMEM((128, 128), BF16),
            pltpu.VMEM((8, 128), F32),
            pltpu.VMEM((7, 128, 128), BF16),
            pltpu.VMEM((7, 8, 128), F32),
            pltpu.VMEM((8, BLOCK, 128), BF16),
            pltpu.VMEM((8, 2, 8, 128), F32),
            pltpu.VMEM((16, 128, 128), BF16),
            pltpu.VMEM((16, 8, 128), F32),
            pltpu.VMEM((128, 128), F32),
            dma(()), dma(()), dma((SENDS,)), dma((SENDS,)), dma((8,)), dma(()), dma(()), dma(()),
            dma((7,)), dma((7,)), dma((7,)), dma((7,)), dma(()), dma(()), dma(()), dma(()), dma((2,)),
        ],
        compiler_params=pltpu.CompilerParams(
            collective_id=0, has_side_effects=True, vmem_limit_bytes=66 * 1000 * 1000
        ),
        name="retention_all",
    )(tokens, w_query, w_key, w_value, w_gate, logd, gain)


def solution(mesh):
    placed = (
        P(("dp", "seq"), "mp"),
        P(None, "mp"),
        P(None, "mp"),
        P(None, "mp"),
        P(None, "mp"),
        P("mp"),
        P(("dp", "seq"), "mp"),
        P(),
    )
    return jax.shard_map(
        body, mesh=mesh, in_specs=placed, out_specs=P(("dp", "seq", "mp"), None), check_vma=False
    )
```

```python
import jax
import jax.numpy as jnp
from jax import lax
from jax.experimental import pallas as pl
from jax.experimental.pallas import tpu as pltpu
from jax.sharding import PartitionSpec as P

DH = 128
CHIPS = 8
BLOCK = 256
BLOCKS = 8
GROUP = 4
MESH = pl.DeviceIdType.MESH
F32 = jnp.float32
BF16 = jnp.bfloat16
PLACE = {0: 0, 1: 1, 7: 2, 2: 3, 6: 4, 3: 5, 5: 6, 4: 7}
ORDER = [0, 1, 7, 2, 6, 3, 5, 4]


def ring_lists():
    right, left = [], []
    for base in range(0, BLOCKS, GROUP):
        even = [base, base + 2, base + 1, base + 3]
        odd = [base + 1, base + 3, base, base + 2]
        for d in (1, 2, 3):
            right += [(j, d) for j in even]
            left += [(j, d) for j in odd]
        right += [(j, 4) for j in even[:2]]
        left += [(j, 4) for j in odd[:2]]
    return right, left


RIGHT, LEFT = ring_lists()
SENDS = len(RIGHT)


def dot(a, b):
    return jnp.dot(a, b, preferred_element_type=F32)


def dot_t(a, b):
    return lax.dot_general(a, b, (((1,), (1,)), ((), ())), preferred_element_type=F32)


def t_dot(a, b):
    return lax.dot_general(a, b, (((0,), (0,)), ((), ())), preferred_element_type=F32)


def kernel(
    tok_hbm, wq_hbm, wk_hbm, wv_hbm, wg_hbm, forget_hbm, exponent_ref, gain_ref, out_ref,
    tok, w, decay, kdec, qdec, ends, sg, qd, vb, kb, olocal, states, start, own_state, own_total,
    got_state, got_total, ubuf, ssbuf, obuf, ssgot, carried, forget,
    tok_sem, w_sem, right_sem, left_sem, pair_sem, sent_right, sent_left, sent_pair,
    state_sem, total_sem, state_sent, total_sent, o_sem, ss_sem, o_sent, ss_sent, self_sem, later_in, forget_sem,
):
    m = lax.axis_index("mp")
    z = lax.axis_index("seq")
    core = lax.rem(m, 2)
    y = m // 2
    pair = m + 1 - 2 * core
    to_right = lax.rem(m + 2, 16)
    to_left = lax.rem(m + 14, 16)

    barrier = pltpu.get_barrier_semaphore()
    for near in (to_left, to_right, pair):
        pl.semaphore_signal(barrier, inc=1, device_id={"mp": near}, device_id_type=MESH)
    for e in range(1, 8):

        @pl.when(z + e < 8)
        def _():
            pl.semaphore_signal(barrier, inc=1, device_id={"seq": lax.rem(z + e, 8)}, device_id_type=MESH)

    def columns(place, of):
        return pl.ds(pl.multiple_of(place * 256 + of * 128, 128), 128)

    own_copy = pltpu.make_async_copy(tok_hbm, tok.at[:, columns(0, core)], tok_sem)
    own_copy.start()
    forget_copy = pltpu.make_async_copy(forget_hbm, forget, forget_sem)
    forget_copy.start()
    for r in ORDER:
        source = pl.ds(pl.multiple_of(lax.rem(y + 8 - r, 8) * 256, 256), 256)
        rows = pl.ds(PLACE[r] * 256, 256)
        for n, weight in enumerate((wk_hbm, wv_hbm, wq_hbm, wg_hbm)):
            pltpu.make_async_copy(weight.at[source], w.at[rows, pl.ds(n * 128, 128)], w_sem).start()

    forget_copy.wait()
    v = jnp.exp2(jnp.full((16, 128), -exponent_ref[0].astype(F32)))
    series = jnp.full((16, 128), 1.0 / 8)
    for n in range(7, 0, -1):
        series = 1.0 / n + v * series
    logd = -v * series - forget[...]
    lane = lax.broadcasted_iota(jnp.int32, (16, 128), 1)
    row = lax.broadcasted_iota(jnp.int32, (16, 128), 0)
    run = logd
    for shift in (1, 2, 4, 8, 16, 32, 64):
        run = run + jnp.where(lane >= shift, pltpu.roll(run, shift, 1), 0.0)
    half_sum = jnp.broadcast_to(run[:, 127:128], (16, 128))
    run = run + jnp.where(row % 2 == 1, pltpu.roll(half_sum, 1, 0), 0.0)
    turned = run.T
    before = jnp.zeros((8, 128), F32)
    for j in range(BLOCKS):
        end = jnp.broadcast_to(run[2 * j + 1 : 2 * j + 2, 127:128], (8, 128))
        ends[0, j] = end
        ends[1, j] = before
        before = before + end
    own_total[...] = before

    pl.semaphore_wait(barrier, 3 + z)
    for e in range(1, 8):

        @pl.when(z >= e)
        def _():
            pl.semaphore_signal(later_in.at[e - 1], inc=1, device_id={"seq": lax.rem(z + 8 - e, 8)}, device_id_type=MESH)

    own_copy.wait()

    def ring_copy(direction, index):
        j, d = (RIGHT if direction > 0 else LEFT)[index]
        source = (d - 1) if direction > 0 else (8 - (d - 1)) % 8
        target = d if direction > 0 else 8 - d
        rows = pl.ds(j * BLOCK, BLOCK)
        return pltpu.make_async_remote_copy(
            src_ref=tok.at[rows, columns(PLACE[source], core)],
            dst_ref=tok.at[rows, columns(PLACE[target], core)],
            send_sem=sent_right if direction > 0 else sent_left,
            recv_sem=(right_sem if direction > 0 else left_sem).at[index],
            device_id={"mp": to_right if direction > 0 else to_left},
            device_id_type=MESH,
        )

    def pair_copy(j, r):
        rows = pl.ds(j * BLOCK, BLOCK)
        spot = tok.at[rows, columns(PLACE[r], core)]
        return pltpu.make_async_remote_copy(
            src_ref=spot, dst_ref=spot, send_sem=sent_pair, recv_sem=pair_sem.at[j],
            device_id={"mp": pair}, device_id_type=MESH,
        )

    for index in range(GROUP):
        ring_copy(1, index).start()
        ring_copy(-1, index).start()
    for j in range(BLOCKS):
        pair_copy(j, 0).start()

    def total_copy(e):
        return pltpu.make_async_remote_copy(
            src_ref=own_total, dst_ref=got_total.at[e - 1], send_sem=total_sent.at[e - 1],
            recv_sem=total_sem.at[e - 1], device_id={"seq": lax.rem(z + e, 8)}, device_id_type=MESH,
        )

    def state_copy(e):
        return pltpu.make_async_remote_copy(
            src_ref=own_state, dst_ref=got_state.at[e - 1], send_sem=state_sent.at[e - 1],
            recv_sem=state_sem.at[e - 1], device_id={"seq": lax.rem(z + e, 8)}, device_id_type=MESH,
        )

    def make_decay(j):
        rows = pl.ds(j * BLOCK, BLOCK)
        down = jnp.concatenate([turned[:, 2 * j : 2 * j + 1], turned[:, 2 * j + 1 : 2 * j + 2]], axis=0)
        across = jnp.concatenate([run[2 * j : 2 * j + 1], run[2 * j + 1 : 2 * j + 2]], axis=1)
        t = lax.broadcasted_iota(jnp.int32, (BLOCK, BLOCK), 0)
        s = lax.broadcasted_iota(jnp.int32, (BLOCK, BLOCK), 1)
        gap = jnp.where(t >= s, down - across, 0.0)
        decay[j] = jnp.where(t >= s, jnp.exp(gap), 0.0)
        wide = jnp.broadcast_to(down, (BLOCK, DH))
        qdec[rows] = jnp.exp(wide)
        kdec[rows] = jnp.exp(ends[0, j, 0:1] - wide)

    def project_kv(j):
        rows = pl.ds(pl.multiple_of(j * BLOCK, BLOCK), BLOCK)
        both = dot(tok[rows], w[:, 0:256])
        keys = (both[:, :128] * DH**-0.5).astype(BF16)
        values = both[:, 128:].astype(BF16)
        kb[rows] = keys
        vb[rows] = values
        faded = (keys.astype(F32) * kdec[rows]).astype(BF16)
        start[j] = carried[...]
        carried[...] = jnp.exp(ends[0, j, 0:1]) * carried[...] + t_dot(faded, values)

    def project_qg(j):
        rows = pl.ds(pl.multiple_of(j * BLOCK, BLOCK), BLOCK)
        both = dot(tok[rows], w[:, 256:512])
        queries = both[:, :128].astype(BF16)
        gate = both[:, 128:].astype(BF16).astype(F32)
        sg[rows] = gate / (1.0 + jnp.exp(-gate)) * gain_ref[pl.ds(m, 1), :]
        qd[rows] = (queries.astype(F32) * qdec[rows]).astype(BF16)
        scores = (dot_t(queries, kb[rows]) * decay[j]).astype(BF16)
        olocal[rows] = dot(scores, vb[rows])

    def wait_weights():
        pltpu.make_async_copy(w, w, w_sem).wait()

    carried[...] = jnp.zeros_like(carried)
    ready = 14
    for index in range(SENDS):
        for direction in (1, -1):
            ring_copy(direction, index).wait_recv()
            if index + GROUP < SENDS:
                ring_copy(direction, index + GROUP).start()
            j, d = (RIGHT if direction > 0 else LEFT)[index]
            pair_copy(j, d if direction > 0 else 8 - d).start()
        if index < BLOCKS:
            make_decay(index)
        if index == ready:
            for e in range(1, 8):

                @pl.when(z + e < 8)
                def _():
                    pl.semaphore_wait(later_in.at[e - 1], 1)
                    total_copy(e).start()

            wait_weights()
            for j in range(GROUP):
                pltpu.make_async_copy(tok.at[pl.ds(0, BLOCK), pl.ds(0, 1024)], tok.at[pl.ds(0, BLOCK), pl.ds(0, 1024)], pair_sem.at[j]).wait()
        piece = index - ready - 1
        if 0 <= piece < 2 * GROUP:
            (project_qg if piece % 2 else project_kv)(piece // 2)

    for j in range(GROUP, BLOCKS):
        pltpu.make_async_copy(tok.at[pl.ds(0, BLOCK), pl.ds(0, 1024)], tok.at[pl.ds(0, BLOCK), pl.ds(0, 1024)], pair_sem.at[j]).wait()

    def each(lower, upper, run_one):
        def step(j, _):
            run_one(j)
            return 0

        lax.fori_loop(lower, upper, step, 0)

    each(GROUP, BLOCKS, project_kv)
    own_state[...] = carried[...].astype(BF16)
    for e in range(1, 8):

        @pl.when(z + e < 8)
        def _():
            state_copy(e).start()

    each(GROUP, BLOCKS, project_qg)

    carried[...] = jnp.zeros_like(carried)
    states[...] = jnp.zeros_like(states)
    for e in range(1, 8):

        @pl.when(z >= e)
        def _():
            total_copy(e).wait_recv()
            state_copy(e).wait_recv()
            carried[...] += jnp.exp(states[0:1]) * got_state[e - 1].astype(F32)
            states[...] += got_total[e - 1]

    one = jnp.ones((8, 128), BF16)

    def out_copy(j, other, r):
        target = 2 * j + other
        return (
            pltpu.make_async_remote_copy(
                src_ref=ubuf.at[j, pl.ds(pl.multiple_of(other * 128, 128), 128)], dst_ref=obuf.at[m], send_sem=o_sent, recv_sem=o_sem,
                device_id={"mp": target}, device_id_type=MESH,
            ),
            pltpu.make_async_remote_copy(
                src_ref=ssbuf.at[j, other], dst_ref=ssgot.at[m], send_sem=ss_sent, recv_sem=ss_sem,
                device_id={"mp": target}, device_id_type=MESH,
            ),
        )

    for r in (4, 3, 5, 2, 6, 1, 7, 0):
        j = lax.rem(y + r, 8)
        rows = pl.ds(pl.multiple_of(j * BLOCK, BLOCK), BLOCK)
        entering = start[j] + jnp.exp(ends[1, j, 0:1]) * carried[...]
        o = (olocal[rows] + dot(qd[rows], entering.astype(BF16))).astype(BF16).astype(F32)
        ubuf[j] = (sg[rows] * o).astype(BF16)
        square = o * o
        high = square.astype(BF16)
        low = (square - high.astype(F32)).astype(BF16)
        total = dot_t(one, high) + dot_t(one, low)
        ssbuf[j, 0] = total[:, :128]
        ssbuf[j, 1] = total[:, 128:]
        if r:
            for other in (0, 1):
                for copy in out_copy(j, other, r):
                    copy.start()
        else:
            for copy in out_copy(j, 1 - core, r):
                copy.start()
            mine = pl.ds(pl.multiple_of(core * 128, 128), 128)
            keep = (
                pltpu.make_async_copy(ubuf.at[j, mine], obuf.at[m], self_sem.at[0]),
                pltpu.make_async_copy(ssbuf.at[j, core], ssgot.at[m], self_sem.at[1]),
            )
            for copy in keep:
                copy.start()
            for copy in keep:
                copy.wait()

    pltpu.make_async_copy(ssgot.at[pl.ds(0, 15)], ssgot.at[pl.ds(0, 15)], ss_sem).wait()
    pltpu.make_async_copy(obuf.at[pl.ds(0, 15)], obuf.at[pl.ds(0, 15)], o_sem).wait()
    squares = ssgot[0]
    for n in range(1, 16):
        squares = squares + ssgot[n]
    rstd = lax.rsqrt(squares / 2048.0 + 1e-06)
    down = jnp.broadcast_to(rstd[0:1], (128, 128)).T
    for n in range(16):
        out_ref[:, n * 128 : (n + 1) * 128] = (obuf[n].astype(F32) * down).astype(BF16)

    for sem in (sent_right, sent_left):
        spot = tok.at[pl.ds(0, SENDS * 16), :]
        pltpu.make_async_copy(spot, spot, sem).wait()
    spot = tok.at[:, pl.ds(0, 1024)]
    pltpu.make_async_copy(spot, spot, sent_pair).wait()
    pltpu.make_async_copy(obuf.at[pl.ds(0, 15)], obuf.at[pl.ds(0, 15)], o_sent).wait()
    pltpu.make_async_copy(ssgot.at[pl.ds(0, 15)], ssgot.at[pl.ds(0, 15)], ss_sent).wait()
    for e in range(1, 8):

        @pl.when(z + e < 8)
        def _():
            total_copy(e).wait_send()
            state_copy(e).wait_send()


def body(tokens, w_query, w_key, w_value, w_gate, decay_exponent, forget, norm_gain):
    gain = norm_gain.reshape(16, 128)
    vmem = pl.BlockSpec(memory_space=pltpu.VMEM)
    anywhere = pl.BlockSpec(memory_space=pl.ANY)
    dma = pltpu.SemaphoreType.DMA
    return pl.pallas_call(
        kernel,
        out_shape=jax.ShapeDtypeStruct((128, 2048), BF16),
        in_specs=[anywhere] * 6 + [pl.BlockSpec(memory_space=pltpu.SMEM), vmem],
        out_specs=vmem,
        scratch_shapes=[
            pltpu.VMEM((2048, 2048), BF16),
            pltpu.VMEM((2048, 512), BF16),
            pltpu.VMEM((8, BLOCK, BLOCK), F32),
            pltpu.VMEM((2048, 128), F32),
            pltpu.VMEM((2048, 128), F32),
            pltpu.VMEM((2, 8, 8, 128), F32),
            pltpu.VMEM((2048, 128), F32),
            pltpu.VMEM((2048, 128), BF16),
            pltpu.VMEM((2048, 128), BF16),
            pltpu.VMEM((2048, 128), BF16),
            pltpu.VMEM((2048, 128), F32),
            pltpu.VMEM((8, 128), F32),
            pltpu.VMEM((8, 128, 128), F32),
            pltpu.VMEM((128, 128), BF16),
            pltpu.VMEM((8, 128), F32),
            pltpu.VMEM((7, 128, 128), BF16),
            pltpu.VMEM((7, 8, 128), F32),
            pltpu.VMEM((8, BLOCK, 128), BF16),
            pltpu.VMEM((8, 2, 8, 128), F32),
            pltpu.VMEM((16, 128, 128), BF16),
            pltpu.VMEM((16, 8, 128), F32),
            pltpu.VMEM((128, 128), F32),
            pltpu.VMEM((16, 128), F32),
            dma(()), dma(()), dma((SENDS,)), dma((SENDS,)), dma((8,)), dma(()), dma(()), dma(()),
            dma((7,)), dma((7,)), dma((7,)), dma((7,)), dma(()), dma(()), dma(()), dma(()), dma((2,)),
            pltpu.SemaphoreType.REGULAR((7,)), dma(()),
        ],
        compiler_params=pltpu.CompilerParams(
            collective_id=0, has_side_effects=True, vmem_limit_bytes=66 * 1000 * 1000
        ),
        name="retention_all",
    )(tokens, w_query, w_key, w_value, w_gate, forget.reshape(16, 128), decay_exponent, gain)


def solution(mesh):
    placed = (
        P(("dp", "seq"), "mp"),
        P(None, "mp"),
        P(None, "mp"),
        P(None, "mp"),
        P(None, "mp"),
        P("mp"),
        P(("dp", "seq"), "mp"),
        P(),
    )
    return jax.shard_map(
        body, mesh=mesh, in_specs=placed, out_specs=P(("dp", "seq", "mp"), None), check_vma=False
    )
```

```python
import jax
import jax.numpy as jnp
from jax import lax
from jax.experimental import pallas as pl
from jax.experimental.pallas import tpu as pltpu
from jax.sharding import PartitionSpec as P

DH = 128
CHIPS = 8
BLOCK = 256
BLOCKS = 8
GROUP = 4
MESH = pl.DeviceIdType.MESH
F32 = jnp.float32
BF16 = jnp.bfloat16
PLACE = {0: 0, 1: 1, 7: 2, 2: 3, 6: 4, 3: 5, 5: 6, 4: 7}
ORDER = [0, 1, 7, 2, 6, 3, 5, 4]


def ring_lists():
    right, left = [], []
    for base in range(0, BLOCKS, GROUP):
        even = [base, base + 2, base + 1, base + 3]
        odd = [base + 1, base + 3, base, base + 2]
        for d in (1, 2, 3):
            right += [(j, d) for j in even]
            left += [(j, d) for j in odd]
        right += [(j, 4) for j in even[:2]]
        left += [(j, 4) for j in odd[:2]]
    return right, left


RIGHT, LEFT = ring_lists()
SENDS = len(RIGHT)
RIGHT_FIRST = [0, 1, 2, 3, 4, 5, 6, 7]
PART = {0: 0, 1: 0, 7: 0, 2: 1, 6: 1, 3: 2, 5: 2, 4: 3}
PLACES = ((0, 3), (3, 5), (5, 7), (7, 8))


def dot(a, b):
    return jnp.dot(a, b, preferred_element_type=F32)


def dot_t(a, b):
    return lax.dot_general(a, b, (((1,), (1,)), ((), ())), preferred_element_type=F32)


def t_dot(a, b):
    return lax.dot_general(a, b, (((0,), (0,)), ((), ())), preferred_element_type=F32)


def kernel(
    tok_hbm, wq_hbm, wk_hbm, wv_hbm, wg_hbm, forget_hbm, exponent_ref, gain_ref, out_ref,
    tok, w, decay, kdec, qdec, ends, sg, qd, vb, kb, olocal, states, start, own_state, own_total,
    got_state, got_total, ubuf, ssbuf, obuf, ssgot, carried, forget, partial,
    tok_sem, w_sem, right_sem, left_sem, pair_sem, sent_right, sent_left, sent_pair,
    state_sem, total_sem, state_sent, total_sent, o_sem, ss_sem, o_sent, ss_sent, self_sem, later_in, forget_sem,
):
    m = lax.axis_index("mp")
    z = lax.axis_index("seq")
    core = lax.rem(m, 2)
    y = m // 2
    pair = m + 1 - 2 * core
    to_right = lax.rem(m + 2, 16)
    to_left = lax.rem(m + 14, 16)

    barrier = pltpu.get_barrier_semaphore()
    for near in (to_left, to_right, pair):
        pl.semaphore_signal(barrier, inc=1, device_id={"mp": near}, device_id_type=MESH)
    for e in range(1, 8):

        @pl.when(z + e < 8)
        def _():
            pl.semaphore_signal(barrier, inc=1, device_id={"seq": lax.rem(z + e, 8)}, device_id_type=MESH)

    def columns(place, of):
        return pl.ds(pl.multiple_of(place * 256 + of * 128, 128), 128)

    def own_copy(j):
        rows = pl.ds(j * BLOCK, BLOCK)
        return pltpu.make_async_copy(tok_hbm.at[rows], tok.at[rows, columns(0, core)], tok_sem.at[j])

    for j in RIGHT_FIRST:
        own_copy(j).start()
    pl.semaphore_wait(barrier, 3 + z)
    for e in range(1, 8):

        @pl.when(z >= e)
        def _():
            pl.semaphore_signal(later_in.at[e - 1], inc=1, device_id={"seq": lax.rem(z + 8 - e, 8)}, device_id_type=MESH)


    def ring_copy(direction, index):
        j, d = (RIGHT if direction > 0 else LEFT)[index]
        source = (d - 1) if direction > 0 else (8 - (d - 1)) % 8
        target = d if direction > 0 else 8 - d
        rows = pl.ds(j * BLOCK, BLOCK)
        return pltpu.make_async_remote_copy(
            src_ref=tok.at[rows, columns(PLACE[source], core)],
            dst_ref=tok.at[rows, columns(PLACE[target], core)],
            send_sem=sent_right if direction > 0 else sent_left,
            recv_sem=(right_sem if direction > 0 else left_sem).at[index],
            device_id={"mp": to_right if direction > 0 else to_left},
            device_id_type=MESH,
        )

    def pair_copy(j, r):
        rows = pl.ds(j * BLOCK, BLOCK)
        spot = tok.at[rows, columns(PLACE[r], core)]
        return pltpu.make_async_remote_copy(
            src_ref=spot, dst_ref=spot, send_sem=sent_pair, recv_sem=pair_sem.at[j, PART[r]],
            device_id={"mp": pair}, device_id_type=MESH,
        )

    for j in range(GROUP):
        own_copy(j).wait()
    for index in range(GROUP):
        ring_copy(1, index).start()
        ring_copy(-1, index).start()
    for j in range(GROUP, BLOCKS):
        own_copy(j).wait()
    for j in range(BLOCKS):
        pair_copy(j, 0).start()

    forget_copy = pltpu.make_async_copy(forget_hbm, forget, forget_sem)
    forget_copy.start()
    for r in ORDER:
        source = pl.ds(pl.multiple_of(lax.rem(y + 8 - r, 8) * 256, 256), 256)
        rows = pl.ds(PLACE[r] * 256, 256)
        for n, weight in enumerate((wk_hbm, wv_hbm, wq_hbm, wg_hbm)):
            pltpu.make_async_copy(weight.at[source], w.at[rows, pl.ds(n * 128, 128)], w_sem).start()

    forget_copy.wait()
    v = jnp.exp2(jnp.full((16, 128), -exponent_ref[0].astype(F32)))
    series = jnp.full((16, 128), 1.0 / 8)
    for n in range(7, 0, -1):
        series = 1.0 / n + v * series
    logd = -v * series - forget[...]
    lane = lax.broadcasted_iota(jnp.int32, (16, 128), 1)
    row = lax.broadcasted_iota(jnp.int32, (16, 128), 0)
    run = logd
    for shift in (1, 2, 4, 8, 16, 32, 64):
        run = run + jnp.where(lane >= shift, pltpu.roll(run, shift, 1), 0.0)
    half_sum = jnp.broadcast_to(run[:, 127:128], (16, 128))
    run = run + jnp.where(row % 2 == 1, pltpu.roll(half_sum, 1, 0), 0.0)
    turned = run.T
    before = jnp.zeros((8, 128), F32)
    for j in range(BLOCKS):
        end = jnp.broadcast_to(run[2 * j + 1 : 2 * j + 2, 127:128], (8, 128))
        ends[0, j] = end
        ends[1, j] = before
        before = before + end
    own_total[...] = before

    def total_copy(e):
        return pltpu.make_async_remote_copy(
            src_ref=own_total, dst_ref=got_total.at[e - 1], send_sem=total_sent.at[e - 1],
            recv_sem=total_sem.at[e - 1], device_id={"seq": lax.rem(z + e, 8)}, device_id_type=MESH,
        )

    def state_copy(e):
        return pltpu.make_async_remote_copy(
            src_ref=own_state, dst_ref=got_state.at[e - 1], send_sem=state_sent.at[e - 1],
            recv_sem=state_sem.at[e - 1], device_id={"seq": lax.rem(z + e, 8)}, device_id_type=MESH,
        )

    def make_decay(j):
        rows = pl.ds(j * BLOCK, BLOCK)
        down = jnp.concatenate([turned[:, 2 * j : 2 * j + 1], turned[:, 2 * j + 1 : 2 * j + 2]], axis=0)
        across = jnp.concatenate([run[2 * j : 2 * j + 1], run[2 * j + 1 : 2 * j + 2]], axis=1)
        t = lax.broadcasted_iota(jnp.int32, (BLOCK, BLOCK), 0)
        s = lax.broadcasted_iota(jnp.int32, (BLOCK, BLOCK), 1)
        gap = jnp.where(t >= s, down - across, 0.0)
        decay[j] = jnp.where(t >= s, jnp.exp(gap), 0.0)
        wide = jnp.broadcast_to(down, (BLOCK, DH))
        qdec[rows] = jnp.exp(wide)
        kdec[rows] = jnp.exp(ends[0, j, 0:1] - wide)

    def project_kv(j):
        rows = pl.ds(pl.multiple_of(j * BLOCK, BLOCK), BLOCK)
        both = dot(tok[rows], w[:, 0:256])
        keys = (both[:, :128] * DH**-0.5).astype(BF16)
        values = both[:, 128:].astype(BF16)
        kb[rows] = keys
        vb[rows] = values
        faded = (keys.astype(F32) * kdec[rows]).astype(BF16)
        start[j] = carried[...]
        carried[...] = jnp.exp(ends[0, j, 0:1]) * carried[...] + t_dot(faded, values)

    def project_qg(j):
        rows = pl.ds(pl.multiple_of(j * BLOCK, BLOCK), BLOCK)
        both = dot(tok[rows], w[:, 256:512])
        queries = both[:, :128].astype(BF16)
        gate = both[:, 128:].astype(BF16).astype(F32)
        sg[rows] = gate / (1.0 + jnp.exp(-gate)) * gain_ref[pl.ds(m, 1), :]
        qd[rows] = (queries.astype(F32) * qdec[rows]).astype(BF16)
        scores = (dot_t(queries, kb[rows]) * decay[j]).astype(BF16)
        olocal[rows] = dot(scores, vb[rows])

    def wait_weights():
        pltpu.make_async_copy(w, w, w_sem).wait()

    def wait_pair(j, part):
        first, last = PLACES[part]
        spot = tok.at[pl.ds(j * BLOCK, BLOCK), pl.ds(0, 128 * (last - first))]
        pltpu.make_async_copy(spot, spot, pair_sem.at[j, part]).wait()

    late = pl.ds(GROUP * BLOCK, GROUP * BLOCK)

    def add_part(j, part):
        wait_pair(j, part)
        first, last = PLACES[part]
        span = pl.ds(first * 256, (last - first) * 256)
        rows = pl.ds((j - GROUP) * BLOCK, BLOCK)
        product = dot(tok[pl.ds(j * BLOCK, BLOCK), span], w[span, :])
        if part:
            partial[rows] += product
        else:
            partial[rows] = product

    carried[...] = jnp.zeros_like(carried)
    ready = 14
    for index in range(SENDS):
        for direction in (1, -1):
            ring_copy(direction, index).wait_recv()
            if index + GROUP < SENDS:
                ring_copy(direction, index + GROUP).start()
            j, d = (RIGHT if direction > 0 else LEFT)[index]
            pair_copy(j, d if direction > 0 else 8 - d).start()
        if index < BLOCKS:
            make_decay(index)
        if index == ready:
            for e in range(1, 8):

                @pl.when(z + e < 8)
                def _():
                    pl.semaphore_wait(later_in.at[e - 1], 1)
                    total_copy(e).start()

            wait_weights()
            for j in range(GROUP):
                for part in range(4):
                    wait_pair(j, part)
        piece = index - ready - 1
        if 0 <= piece < 2 * GROUP:
            (project_qg if piece % 2 else project_kv)(piece // 2)
        if 20 <= index < 24:
            add_part(GROUP + index - 20, 0)
        if index in (24, 25):
            add_part(GROUP + 2 * (index - 24), 1)
            add_part(GROUP + 2 * (index - 24) + 1, 1)
        if index == 26:
            for j in range(GROUP, BLOCKS):
                add_part(j, 2)

    for j in range(GROUP, BLOCKS):
        wait_pair(j, 3)
    far = tok[late, 1792:2048]
    both = partial[:, :256] + dot(far, w[1792:2048, :256])
    keys = (both[:, :128] * DH**-0.5).astype(BF16)
    values = both[:, 128:].astype(BF16)
    kb[late] = keys
    vb[late] = values
    faded = (keys.astype(F32) * kdec[late]).astype(BF16)
    added = [
        t_dot(faded[n * BLOCK : (n + 1) * BLOCK], values[n * BLOCK : (n + 1) * BLOCK]) for n in range(GROUP)
    ]
    state = carried[...]
    for n in range(GROUP):
        start[GROUP + n] = state
        state = jnp.exp(ends[0, GROUP + n, 0:1]) * state + added[n]
    own_state[...] = state.astype(BF16)
    for e in range(1, 8):

        @pl.when(z + e < 8)
        def _():
            state_copy(e).start()

    both = partial[:, 256:] + dot(tok[late, 1792:2048], w[1792:2048, 256:])
    queries = both[:, :128].astype(BF16)
    gate = both[:, 128:].astype(BF16).astype(F32)
    sg[late] = gate / (1.0 + jnp.exp(-gate)) * gain_ref[pl.ds(m, 1), :]
    qd[late] = (queries.astype(F32) * qdec[late]).astype(BF16)
    for n in range(GROUP):
        rows = pl.ds((GROUP + n) * BLOCK, BLOCK)
        scores = (dot_t(queries[n * BLOCK : (n + 1) * BLOCK], kb[rows]) * decay[GROUP + n]).astype(BF16)
        olocal[rows] = dot(scores, vb[rows])

    carried[...] = jnp.zeros_like(carried)
    states[...] = jnp.zeros_like(states)
    for e in range(1, 8):

        @pl.when(z >= e)
        def _():
            total_copy(e).wait_recv()
            state_copy(e).wait_recv()
            carried[...] += jnp.exp(states[0:1]) * got_state[e - 1].astype(F32)
            states[...] += got_total[e - 1]

    one = jnp.ones((8, 128), BF16)

    def out_copy(j, other, r):
        target = 2 * j + other
        return (
            pltpu.make_async_remote_copy(
                src_ref=ubuf.at[j, pl.ds(pl.multiple_of(other * 128, 128), 128)], dst_ref=obuf.at[m], send_sem=o_sent, recv_sem=o_sem,
                device_id={"mp": target}, device_id_type=MESH,
            ),
            pltpu.make_async_remote_copy(
                src_ref=ssbuf.at[j, other, pl.ds(0, 1)], dst_ref=ssgot.at[m, pl.ds(0, 1)], send_sem=ss_sent, recv_sem=ss_sem,
                device_id={"mp": target}, device_id_type=MESH,
            ),
        )

    for r in (4, 3, 5, 2, 6, 1, 7, 0):
        j = lax.rem(y + r, 8)
        rows = pl.ds(pl.multiple_of(j * BLOCK, BLOCK), BLOCK)
        entering = start[j] + jnp.exp(ends[1, j, 0:1]) * carried[...]
        o = (olocal[rows] + dot(qd[rows], entering.astype(BF16))).astype(BF16).astype(F32)
        ubuf[j] = (sg[rows] * o).astype(BF16)
        square = o * o
        high = square.astype(BF16)
        low = (square - high.astype(F32)).astype(BF16)
        total = dot_t(one, high) + dot_t(one, low)
        ssbuf[j, 0] = total[:, :128]
        ssbuf[j, 1] = total[:, 128:]
        if r:
            for other in (0, 1):
                for copy in out_copy(j, other, r):
                    copy.start()
        else:
            for copy in out_copy(j, 1 - core, r):
                copy.start()
            mine = pl.ds(pl.multiple_of(core * 128, 128), 128)
            keep = (
                pltpu.make_async_copy(ubuf.at[j, mine], obuf.at[m], self_sem.at[0]),
                pltpu.make_async_copy(ssbuf.at[j, core, pl.ds(0, 1)], ssgot.at[m, pl.ds(0, 1)], self_sem.at[1]),
            )
            for copy in keep:
                copy.start()
            for copy in keep:
                copy.wait()

    pltpu.make_async_copy(ssgot.at[pl.ds(0, 15), pl.ds(0, 1)], ssgot.at[pl.ds(0, 15), pl.ds(0, 1)], ss_sem).wait()
    pltpu.make_async_copy(obuf.at[pl.ds(0, 15)], obuf.at[pl.ds(0, 15)], o_sem).wait()
    squares = ssgot[0, 0:1]
    for n in range(1, 16):
        squares = squares + ssgot[n, 0:1]
    rstd = lax.rsqrt(squares / 2048.0 + 1e-06)
    down = jnp.broadcast_to(rstd, (128, 128)).T
    for n in range(16):
        out_ref[:, n * 128 : (n + 1) * 128] = (obuf[n].astype(F32) * down).astype(BF16)

    for sem in (sent_right, sent_left):
        spot = tok.at[pl.ds(0, SENDS * 16), :]
        pltpu.make_async_copy(spot, spot, sem).wait()
    spot = tok.at[:, pl.ds(0, 1024)]
    pltpu.make_async_copy(spot, spot, sent_pair).wait()
    pltpu.make_async_copy(obuf.at[pl.ds(0, 15)], obuf.at[pl.ds(0, 15)], o_sent).wait()
    pltpu.make_async_copy(ssgot.at[pl.ds(0, 15), pl.ds(0, 1)], ssgot.at[pl.ds(0, 15), pl.ds(0, 1)], ss_sent).wait()
    for e in range(1, 8):

        @pl.when(z + e < 8)
        def _():
            total_copy(e).wait_send()
            state_copy(e).wait_send()


def body(tokens, w_query, w_key, w_value, w_gate, decay_exponent, forget, norm_gain):
    gain = norm_gain.reshape(16, 128)
    vmem = pl.BlockSpec(memory_space=pltpu.VMEM)
    anywhere = pl.BlockSpec(memory_space=pl.ANY)
    dma = pltpu.SemaphoreType.DMA
    return pl.pallas_call(
        kernel,
        out_shape=jax.ShapeDtypeStruct((128, 2048), BF16),
        in_specs=[anywhere] * 6 + [pl.BlockSpec(memory_space=pltpu.SMEM), vmem],
        out_specs=vmem,
        scratch_shapes=[
            pltpu.VMEM((2048, 2048), BF16),
            pltpu.VMEM((2048, 512), BF16),
            pltpu.VMEM((8, BLOCK, BLOCK), F32),
            pltpu.VMEM((2048, 128), F32),
            pltpu.VMEM((2048, 128), F32),
            pltpu.VMEM((2, 8, 8, 128), F32),
            pltpu.VMEM((2048, 128), F32),
            pltpu.VMEM((2048, 128), BF16),
            pltpu.VMEM((2048, 128), BF16),
            pltpu.VMEM((2048, 128), BF16),
            pltpu.VMEM((2048, 128), F32),
            pltpu.VMEM((8, 128), F32),
            pltpu.VMEM((8, 128, 128), F32),
            pltpu.VMEM((128, 128), BF16),
            pltpu.VMEM((8, 128), F32),
            pltpu.VMEM((7, 128, 128), BF16),
            pltpu.VMEM((7, 8, 128), F32),
            pltpu.VMEM((8, BLOCK, 128), BF16),
            pltpu.VMEM((8, 2, 8, 128), F32),
            pltpu.VMEM((16, 128, 128), BF16),
            pltpu.VMEM((16, 8, 128), F32),
            pltpu.VMEM((128, 128), F32),
            pltpu.VMEM((16, 128), F32),
            pltpu.VMEM((GROUP * BLOCK, 512), F32),
            dma((8,)), dma(()), dma((SENDS,)), dma((SENDS,)), dma((8, 4)), dma(()), dma(()), dma(()),
            dma((7,)), dma((7,)), dma((7,)), dma((7,)), dma(()), dma(()), dma(()), dma(()), dma((2,)),
            pltpu.SemaphoreType.REGULAR((7,)), dma(()),
        ],
        compiler_params=pltpu.CompilerParams(
            collective_id=0, has_side_effects=True, vmem_limit_bytes=66 * 1000 * 1000
        ),
        name="retention_all",
    )(tokens, w_query, w_key, w_value, w_gate, forget.reshape(16, 128), decay_exponent, gain)


def solution(mesh):
    placed = (
        P(("dp", "seq"), "mp"),
        P(None, "mp"),
        P(None, "mp"),
        P(None, "mp"),
        P(None, "mp"),
        P("mp"),
        P(("dp", "seq"), "mp"),
        P(),
    )
    return jax.shard_map(
        body, mesh=mesh, in_specs=placed, out_specs=P(("dp", "seq", "mp"), None), check_vma=False
    )
```

```python
import jax
import jax.numpy as jnp
from jax import lax
from jax.experimental import pallas as pl
from jax.experimental.pallas import tpu as pltpu
from jax.sharding import PartitionSpec as P

DH = 128
CHIPS = 8
BLOCK = 256
BLOCKS = 8
GROUP = 4
MESH = pl.DeviceIdType.MESH
F32 = jnp.float32
BF16 = jnp.bfloat16
PLACE = {0: 0, 1: 1, 7: 2, 2: 3, 6: 4, 3: 5, 5: 6, 4: 7}
ORDER = [0, 1, 7, 2, 6, 3, 5, 4]


def ring_lists():
    right, left = [], []
    for base in range(0, BLOCKS, GROUP):
        even = [base, base + 2, base + 1, base + 3]
        odd = [base + 1, base + 3, base, base + 2]
        for d in (1, 2, 3):
            right += [(j, d) for j in even]
            left += [(j, d) for j in odd]
        right += [(j, 4) for j in even[:2]]
        left += [(j, 4) for j in odd[:2]]
    return right, left


RIGHT, LEFT = ring_lists()
SENDS = len(RIGHT)
RIGHT_FIRST = [0, 1, 2, 3, 4, 5, 6, 7]
PART = {0: 0, 1: 0, 7: 0, 2: 1, 6: 1, 3: 2, 5: 2, 4: 3}
PLACES = ((0, 3), (3, 5), (5, 7), (7, 8))


def dot(a, b):
    return jnp.dot(a, b, preferred_element_type=F32)


def dot_t(a, b):
    return lax.dot_general(a, b, (((1,), (1,)), ((), ())), preferred_element_type=F32)


def t_dot(a, b):
    return lax.dot_general(a, b, (((0,), (0,)), ((), ())), preferred_element_type=F32)


def kernel(
    tok_hbm, wq_hbm, wk_hbm, wv_hbm, wg_hbm, forget_hbm, exponent_ref, gain_hbm, out_ref, down_ref,
    tok, w, decay, kdec, qdec, ends, sg, qd, vb, kb, olocal, states, start, own_state, own_total,
    got_state, got_total, ubuf, ssbuf, ssgot, carried, forget, partial, gain_ref,
    tok_sem, w_sem, right_sem, left_sem, pair_sem, sent_right, sent_left, sent_pair,
    state_sem, total_sem, state_sent, total_sent, o_sem, ss_sem, o_sent, ss_sent, self_sem, later_in, forget_sem, gain_sem,
):
    m = lax.axis_index("mp")
    z = lax.axis_index("seq")
    core = lax.rem(m, 2)
    y = m // 2
    pair = m + 1 - 2 * core
    to_right = lax.rem(m + 2, 16)
    to_left = lax.rem(m + 14, 16)

    barrier = pltpu.get_barrier_semaphore()
    for near in (to_left, to_right, pair):
        pl.semaphore_signal(barrier, inc=1, device_id={"mp": near}, device_id_type=MESH)
    for e in range(1, 8):

        @pl.when(z + e < 8)
        def _():
            pl.semaphore_signal(barrier, inc=1, device_id={"seq": lax.rem(z + e, 8)}, device_id_type=MESH)

    def columns(place, of):
        return pl.ds(pl.multiple_of(place * 256 + of * 128, 128), 128)

    def own_copy(j):
        rows = pl.ds(j * BLOCK, BLOCK)
        return pltpu.make_async_copy(tok_hbm.at[rows], tok.at[rows, columns(0, core)], tok_sem.at[j])

    for j in RIGHT_FIRST:
        own_copy(j).start()
    pl.semaphore_wait(barrier, 3 + z)
    for e in range(1, 8):

        @pl.when(z >= e)
        def _():
            pl.semaphore_signal(later_in.at[e - 1], inc=1, device_id={"seq": lax.rem(z + 8 - e, 8)}, device_id_type=MESH)


    def ring_copy(direction, index):
        j, d = (RIGHT if direction > 0 else LEFT)[index]
        source = (d - 1) if direction > 0 else (8 - (d - 1)) % 8
        target = d if direction > 0 else 8 - d
        rows = pl.ds(j * BLOCK, BLOCK)
        return pltpu.make_async_remote_copy(
            src_ref=tok.at[rows, columns(PLACE[source], core)],
            dst_ref=tok.at[rows, columns(PLACE[target], core)],
            send_sem=sent_right if direction > 0 else sent_left,
            recv_sem=(right_sem if direction > 0 else left_sem).at[index],
            device_id={"mp": to_right if direction > 0 else to_left},
            device_id_type=MESH,
        )

    def pair_copy(j, r):
        rows = pl.ds(j * BLOCK, BLOCK)
        spot = tok.at[rows, columns(PLACE[r], core)]
        return pltpu.make_async_remote_copy(
            src_ref=spot, dst_ref=spot, send_sem=sent_pair, recv_sem=pair_sem.at[j, PART[r]],
            device_id={"mp": pair}, device_id_type=MESH,
        )

    for j in range(GROUP):
        own_copy(j).wait()
    for index in range(GROUP):
        ring_copy(1, index).start()
        ring_copy(-1, index).start()
    for j in range(GROUP, BLOCKS):
        own_copy(j).wait()
    for j in range(BLOCKS):
        pair_copy(j, 0).start()

    forget_copy = pltpu.make_async_copy(forget_hbm, forget, forget_sem)
    forget_copy.start()
    gain_copy = pltpu.make_async_copy(gain_hbm, gain_ref, gain_sem)
    gain_copy.start()
    for r in ORDER:
        source = pl.ds(pl.multiple_of(lax.rem(y + 8 - r, 8) * 256, 256), 256)
        rows = pl.ds(PLACE[r] * 256, 256)
        for n, weight in enumerate((wk_hbm, wv_hbm, wq_hbm, wg_hbm)):
            pltpu.make_async_copy(weight.at[source], w.at[rows, pl.ds(n * 128, 128)], w_sem).start()

    forget_copy.wait()
    gain_copy.wait()
    v = jnp.exp2(jnp.full((16, 128), -exponent_ref[0].astype(F32)))
    series = jnp.full((16, 128), 1.0 / 8)
    for n in range(7, 0, -1):
        series = 1.0 / n + v * series
    logd = -v * series - forget[...]
    lane = lax.broadcasted_iota(jnp.int32, (16, 128), 1)
    row = lax.broadcasted_iota(jnp.int32, (16, 128), 0)
    run = logd
    for shift in (1, 2, 4, 8, 16, 32, 64):
        run = run + jnp.where(lane >= shift, pltpu.roll(run, shift, 1), 0.0)
    half_sum = jnp.broadcast_to(run[:, 127:128], (16, 128))
    run = run + jnp.where(row % 2 == 1, pltpu.roll(half_sum, 1, 0), 0.0)
    turned = run.T
    before = jnp.zeros((8, 128), F32)
    for j in range(BLOCKS):
        end = jnp.broadcast_to(run[2 * j + 1 : 2 * j + 2, 127:128], (8, 128))
        ends[0, j] = end
        ends[1, j] = before
        before = before + end
    own_total[...] = before

    def total_copy(e):
        return pltpu.make_async_remote_copy(
            src_ref=own_total, dst_ref=got_total.at[e - 1], send_sem=total_sent.at[e - 1],
            recv_sem=total_sem.at[e - 1], device_id={"seq": lax.rem(z + e, 8)}, device_id_type=MESH,
        )

    def state_copy(e):
        return pltpu.make_async_remote_copy(
            src_ref=own_state, dst_ref=got_state.at[e - 1], send_sem=state_sent.at[e - 1],
            recv_sem=state_sem.at[e - 1], device_id={"seq": lax.rem(z + e, 8)}, device_id_type=MESH,
        )

    def make_decay(j):
        rows = pl.ds(j * BLOCK, BLOCK)
        down = jnp.concatenate([turned[:, 2 * j : 2 * j + 1], turned[:, 2 * j + 1 : 2 * j + 2]], axis=0)
        across = jnp.concatenate([run[2 * j : 2 * j + 1], run[2 * j + 1 : 2 * j + 2]], axis=1)
        t = lax.broadcasted_iota(jnp.int32, (BLOCK, BLOCK), 0)
        s = lax.broadcasted_iota(jnp.int32, (BLOCK, BLOCK), 1)
        gap = jnp.where(t >= s, down - across, 0.0)
        decay[j] = jnp.where(t >= s, jnp.exp(gap), 0.0)
        wide = jnp.broadcast_to(down, (BLOCK, DH))
        qdec[rows] = jnp.exp(wide)
        kdec[rows] = jnp.exp(ends[0, j, 0:1] - wide)

    def project_kv(j):
        rows = pl.ds(pl.multiple_of(j * BLOCK, BLOCK), BLOCK)
        both = dot(tok[rows], w[:, 0:256])
        keys = (both[:, :128] * DH**-0.5).astype(BF16)
        values = both[:, 128:].astype(BF16)
        kb[rows] = keys
        vb[rows] = values
        faded = (keys.astype(F32) * kdec[rows]).astype(BF16)
        start[j] = carried[...]
        carried[...] = jnp.exp(ends[0, j, 0:1]) * carried[...] + t_dot(faded, values)

    def project_qg(j):
        rows = pl.ds(pl.multiple_of(j * BLOCK, BLOCK), BLOCK)
        both = dot(tok[rows], w[:, 256:512])
        queries = both[:, :128].astype(BF16)
        gate = both[:, 128:].astype(BF16).astype(F32)
        sg[rows] = gate / (1.0 + jnp.exp(-gate)) * gain_ref[pl.ds(m, 1), :]
        qd[rows] = (queries.astype(F32) * qdec[rows]).astype(BF16)
        scores = (dot_t(queries, kb[rows]) * decay[j]).astype(BF16)
        olocal[rows] = dot(scores, vb[rows])

    def wait_weights():
        pltpu.make_async_copy(w, w, w_sem).wait()

    def wait_pair(j, part):
        first, last = PLACES[part]
        spot = tok.at[pl.ds(j * BLOCK, BLOCK), pl.ds(0, 128 * (last - first))]
        pltpu.make_async_copy(spot, spot, pair_sem.at[j, part]).wait()

    late = pl.ds(GROUP * BLOCK, GROUP * BLOCK)

    def add_part(j, part):
        wait_pair(j, part)
        first, last = PLACES[part]
        span = pl.ds(first * 256, (last - first) * 256)
        rows = pl.ds((j - GROUP) * BLOCK, BLOCK)
        product = dot(tok[pl.ds(j * BLOCK, BLOCK), span], w[span, :])
        if part:
            partial[rows] += product
        else:
            partial[rows] = product

    carried[...] = jnp.zeros_like(carried)
    ready = 14
    for index in range(SENDS):
        for direction in (1, -1):
            ring_copy(direction, index).wait_recv()
            if index + GROUP < SENDS:
                ring_copy(direction, index + GROUP).start()
            j, d = (RIGHT if direction > 0 else LEFT)[index]
            pair_copy(j, d if direction > 0 else 8 - d).start()
        if index < BLOCKS:
            make_decay(index)
        if index == ready:
            for e in range(1, 8):

                @pl.when(z + e < 8)
                def _():
                    pl.semaphore_wait(later_in.at[e - 1], 1)
                    total_copy(e).start()

            wait_weights()
            for j in range(GROUP):
                for part in range(4):
                    wait_pair(j, part)
        piece = index - ready - 1
        if 0 <= piece < 2 * GROUP:
            (project_qg if piece % 2 else project_kv)(piece // 2)
        if 20 <= index < 24:
            add_part(GROUP + index - 20, 0)
        if index in (24, 25):
            add_part(GROUP + 2 * (index - 24), 1)
            add_part(GROUP + 2 * (index - 24) + 1, 1)
        if index == 26:
            for j in range(GROUP, BLOCKS):
                add_part(j, 2)

    for j in range(GROUP, BLOCKS):
        wait_pair(j, 3)
    far = tok[late, 1792:2048]
    both = partial[:, :256] + dot(far, w[1792:2048, :256])
    keys = (both[:, :128] * DH**-0.5).astype(BF16)
    values = both[:, 128:].astype(BF16)
    kb[late] = keys
    vb[late] = values
    faded = (keys.astype(F32) * kdec[late]).astype(BF16)
    added = [
        t_dot(faded[n * BLOCK : (n + 1) * BLOCK], values[n * BLOCK : (n + 1) * BLOCK]) for n in range(GROUP)
    ]
    state = carried[...]
    for n in range(GROUP):
        start[GROUP + n] = state
        state = jnp.exp(ends[0, GROUP + n, 0:1]) * state + added[n]
    own_state[...] = state.astype(BF16)
    for e in range(7, 0, -1):

        @pl.when(z + e < 8)
        def _():
            state_copy(e).start()

    both = partial[:, 256:] + dot(tok[late, 1792:2048], w[1792:2048, 256:])
    queries = both[:, :128].astype(BF16)
    gate = both[:, 128:].astype(BF16).astype(F32)
    sg[late] = gate / (1.0 + jnp.exp(-gate)) * gain_ref[pl.ds(m, 1), :]
    qd[late] = (queries.astype(F32) * qdec[late]).astype(BF16)
    for n in range(GROUP):
        rows = pl.ds((GROUP + n) * BLOCK, BLOCK)
        scores = (dot_t(queries[n * BLOCK : (n + 1) * BLOCK], kb[rows]) * decay[GROUP + n]).astype(BF16)
        olocal[rows] = dot(scores, vb[rows])

    carried[...] = jnp.zeros_like(carried)
    states[...] = jnp.zeros_like(states)
    for e in range(1, 8):

        @pl.when(z >= e)
        def _():
            total_copy(e).wait_recv()
            state_copy(e).wait_recv()
            carried[...] += jnp.exp(states[0:1]) * got_state[e - 1].astype(F32)
            states[...] += got_total[e - 1]

    one = jnp.ones((8, 128), BF16)

    def out_copy(j, other, r):
        target = 2 * j + other
        return (
            pltpu.make_async_remote_copy(
                src_ref=ubuf.at[j, pl.ds(pl.multiple_of(other * 128, 128), 128)], dst_ref=out_ref.at[:, pl.ds(pl.multiple_of(m * 128, 128), 128)], send_sem=o_sent, recv_sem=o_sem,
                device_id={"mp": target}, device_id_type=MESH,
            ),
            pltpu.make_async_remote_copy(
                src_ref=ssbuf.at[j, other, pl.ds(0, 1)], dst_ref=ssgot.at[m, pl.ds(0, 1)], send_sem=ss_sent, recv_sem=ss_sem,
                device_id={"mp": target}, device_id_type=MESH,
            ),
        )

    for r in (4, 3, 5, 2, 6, 1, 7, 0):
        j = lax.rem(y + r, 8)
        rows = pl.ds(pl.multiple_of(j * BLOCK, BLOCK), BLOCK)
        entering = start[j] + jnp.exp(ends[1, j, 0:1]) * carried[...]
        o = (olocal[rows] + dot(qd[rows], entering.astype(BF16))).astype(BF16).astype(F32)
        ubuf[j] = (sg[rows] * o).astype(BF16)
        square = o * o
        high = square.astype(BF16)
        low = (square - high.astype(F32)).astype(BF16)
        total = dot_t(one, high) + dot_t(one, low)
        ssbuf[j, 0] = total[:, :128]
        ssbuf[j, 1] = total[:, 128:]
        if r:
            for other in (0, 1):
                for copy in out_copy(j, other, r):
                    copy.start()
        else:
            for copy in out_copy(j, 1 - core, r):
                copy.start()
            mine = pl.ds(pl.multiple_of(core * 128, 128), 128)
            keep = (
                pltpu.make_async_copy(ubuf.at[j, mine], out_ref.at[:, pl.ds(pl.multiple_of(m * 128, 128), 128)], self_sem.at[0]),
                pltpu.make_async_copy(ssbuf.at[j, core, pl.ds(0, 1)], ssgot.at[m, pl.ds(0, 1)], self_sem.at[1]),
            )
            for copy in keep:
                copy.start()
            for copy in keep:
                copy.wait()

    pltpu.make_async_copy(ssgot.at[pl.ds(0, 15), pl.ds(0, 1)], ssgot.at[pl.ds(0, 15), pl.ds(0, 1)], ss_sem).wait()
    pltpu.make_async_copy(out_ref.at[:, pl.ds(0, 1920)], out_ref.at[:, pl.ds(0, 1920)], o_sem).wait()
    squares = ssgot[0, 0:1]
    for n in range(1, 16):
        squares = squares + ssgot[n, 0:1]
    rstd = lax.rsqrt(squares / 2048.0 + 1e-06)
    down_ref[...] = jnp.broadcast_to(rstd, (128, 128)).T

    for sem in (sent_right, sent_left):
        spot = tok.at[pl.ds(0, SENDS * 16), :]
        pltpu.make_async_copy(spot, spot, sem).wait()
    spot = tok.at[:, pl.ds(0, 1024)]
    pltpu.make_async_copy(spot, spot, sent_pair).wait()
    pltpu.make_async_copy(out_ref.at[:, pl.ds(0, 1920)], out_ref.at[:, pl.ds(0, 1920)], o_sent).wait()
    pltpu.make_async_copy(ssgot.at[pl.ds(0, 15), pl.ds(0, 1)], ssgot.at[pl.ds(0, 15), pl.ds(0, 1)], ss_sent).wait()
    for e in range(1, 8):

        @pl.when(z + e < 8)
        def _():
            total_copy(e).wait_send()
            state_copy(e).wait_send()


def body(tokens, w_query, w_key, w_value, w_gate, decay_exponent, forget, norm_gain):
    gain = norm_gain.reshape(16, 128)
    vmem = pl.BlockSpec(memory_space=pltpu.VMEM)
    anywhere = pl.BlockSpec(memory_space=pl.ANY)
    dma = pltpu.SemaphoreType.DMA
    raw, down = pl.pallas_call(
        kernel,
        out_shape=(pltpu.VMEM((128, 2048), BF16), pltpu.VMEM((128, 128), F32)),
        in_specs=[anywhere] * 6 + [pl.BlockSpec(memory_space=pltpu.SMEM), anywhere],
        out_specs=(vmem, vmem),
        scratch_shapes=[
            pltpu.VMEM((2048, 2048), BF16),
            pltpu.VMEM((2048, 512), BF16),
            pltpu.VMEM((8, BLOCK, BLOCK), F32),
            pltpu.VMEM((2048, 128), F32),
            pltpu.VMEM((2048, 128), F32),
            pltpu.VMEM((2, 8, 8, 128), F32),
            pltpu.VMEM((2048, 128), F32),
            pltpu.VMEM((2048, 128), BF16),
            pltpu.VMEM((2048, 128), BF16),
            pltpu.VMEM((2048, 128), BF16),
            pltpu.VMEM((2048, 128), F32),
            pltpu.VMEM((8, 128), F32),
            pltpu.VMEM((8, 128, 128), F32),
            pltpu.VMEM((128, 128), BF16),
            pltpu.VMEM((8, 128), F32),
            pltpu.VMEM((7, 128, 128), BF16),
            pltpu.VMEM((7, 8, 128), F32),
            pltpu.VMEM((8, BLOCK, 128), BF16),
            pltpu.VMEM((8, 2, 8, 128), F32),
            pltpu.VMEM((16, 8, 128), F32),
            pltpu.VMEM((128, 128), F32),
            pltpu.VMEM((16, 128), F32),
            pltpu.VMEM((GROUP * BLOCK, 512), F32),
            pltpu.VMEM((16, 128), F32),
            dma((8,)), dma(()), dma((SENDS,)), dma((SENDS,)), dma((8, 4)), dma(()), dma(()), dma(()),
            dma((7,)), dma((7,)), dma((7,)), dma((7,)), dma(()), dma(()), dma(()), dma(()), dma((2,)),
            pltpu.SemaphoreType.REGULAR((7,)), dma(()), dma(()),
        ],
        compiler_params=pltpu.CompilerParams(
            collective_id=0, has_side_effects=True, vmem_limit_bytes=67043328 - 1100 * 1024
        ),
        name="retention_all",
    )(tokens, w_query, w_key, w_value, w_gate, forget.reshape(16, 128), decay_exponent, gain)
    return (raw.astype(F32) * down[:, :1]).astype(BF16)


def solution(mesh):
    placed = (
        P(("dp", "seq"), "mp"),
        P(None, "mp"),
        P(None, "mp"),
        P(None, "mp"),
        P(None, "mp"),
        P("mp"),
        P(("dp", "seq"), "mp"),
        P(),
    )
    return jax.shard_map(
        body, mesh=mesh, in_specs=placed, out_specs=P(("dp", "seq", "mp"), None), check_vma=False
    )
```

```python
import jax
import jax.numpy as jnp
from jax import lax
from jax.experimental import pallas as pl
from jax.experimental.pallas import tpu as pltpu
from jax.sharding import PartitionSpec as P

DH = 128
CHIPS = 8
BLOCK = 256
BLOCKS = 8
GROUP = 4
MESH = pl.DeviceIdType.MESH
F32 = jnp.float32
BF16 = jnp.bfloat16
PLACE = {0: 0, 1: 1, 7: 2, 2: 3, 6: 4, 3: 5, 5: 6, 4: 7}
ORDER = [0, 1, 7, 2, 6, 3, 5, 4]


def ring_lists():
    near, far = [0, 2, 1, 3], [4, 6, 5, 7]
    order = [(j, 1) for j in near] + [(j, 1) for j in far[:2]]
    order += [(j, 2) for j in near] + [(j, 1) for j in far[2:]]
    order += [(j, 3) for j in near] + [(j, 2) for j in far[:2]]
    order += [(j, 4) for j in near[:2]] + [(j, 2) for j in far[2:]]
    order += [(j, 3) for j in far] + [(j, 4) for j in far[:2]]
    return order, [(j + 1 - 2 * (j % 2), d) for j, d in order]


RIGHT, LEFT = ring_lists()
FLIGHT = 6
START = [max(n - FLIGHT, RIGHT.index((j, d - 1)) if d > 1 else -1) for n, (j, d) in enumerate(RIGHT)]
SENDS = len(RIGHT)
PART = {0: 0, 1: 0, 7: 0, 2: 1, 6: 1, 3: 2, 5: 2, 4: 3}
PLACES = ((0, 3), (3, 5), (5, 7), (7, 8))


def dot(a, b):
    return jnp.dot(a, b, preferred_element_type=F32)


def dot_t(a, b):
    return lax.dot_general(a, b, (((1,), (1,)), ((), ())), preferred_element_type=F32)


def t_dot(a, b):
    return lax.dot_general(a, b, (((0,), (0,)), ((), ())), preferred_element_type=F32)


def kernel(
    tok_hbm, wq_hbm, wk_hbm, wv_hbm, wg_hbm, forget_hbm, exponent_ref, gain_hbm, out_ref, down_ref,
    tok, w, decay, kdec, qdec, ends, sg, qd, vb, kb, olocal, states, start, own_state, own_total,
    got_state, got_total, ubuf, ssbuf, ssgot, carried, forget, partial, gain_ref,
    tok_sem, w_sem, right_sem, left_sem, pair_sem, sent_right, sent_left, sent_pair,
    state_sem, total_sem, state_sent, total_sent, o_sem, ss_sem, o_sent, ss_sent, self_sem, later_in, forget_sem, gain_sem,
):
    m = lax.axis_index("mp")
    z = lax.axis_index("seq")
    core = lax.rem(m, 2)
    y = m // 2
    pair = m + 1 - 2 * core
    to_right = lax.rem(m + 2, 16)
    to_left = lax.rem(m + 14, 16)

    def columns(place, of):
        return pl.ds(pl.multiple_of(place * 256 + of * 128, 128), 128)

    def own_copy(j):
        rows = pl.ds(j * BLOCK, BLOCK)
        return pltpu.make_async_copy(tok_hbm.at[rows], tok.at[rows, columns(0, core)], tok_sem.at[j])

    for j in (0, 2, 1, 3, 4, 6, 5, 7):
        own_copy(j).start()

    barrier = pltpu.get_barrier_semaphore()
    for near in (to_left, to_right, pair):
        pl.semaphore_signal(barrier, inc=1, device_id={"mp": near}, device_id_type=MESH)
    for e in range(1, 8):

        @pl.when(z + e < 8)
        def _():
            pl.semaphore_signal(barrier, inc=1, device_id={"seq": lax.rem(z + e, 8)}, device_id_type=MESH)
    pl.semaphore_wait(barrier, 3 + z)
    for e in range(1, 8):

        @pl.when(z >= e)
        def _():
            pl.semaphore_signal(later_in.at[e - 1], inc=1, device_id={"seq": lax.rem(z + 8 - e, 8)}, device_id_type=MESH)


    def ring_copy(direction, index):
        j, d = (RIGHT if direction > 0 else LEFT)[index]
        source = (d - 1) if direction > 0 else (8 - (d - 1)) % 8
        target = d if direction > 0 else 8 - d
        rows = pl.ds(j * BLOCK, BLOCK)
        return pltpu.make_async_remote_copy(
            src_ref=tok.at[rows, columns(PLACE[source], core)],
            dst_ref=tok.at[rows, columns(PLACE[target], core)],
            send_sem=sent_right if direction > 0 else sent_left,
            recv_sem=(right_sem if direction > 0 else left_sem).at[index],
            device_id={"mp": to_right if direction > 0 else to_left},
            device_id_type=MESH,
        )

    def pair_copy(j, r):
        rows = pl.ds(j * BLOCK, BLOCK)
        spot = tok.at[rows, columns(PLACE[r], core)]
        return pltpu.make_async_remote_copy(
            src_ref=spot, dst_ref=spot, send_sem=sent_pair, recv_sem=pair_sem.at[j, PART[r]],
            device_id={"mp": pair}, device_id_type=MESH,
        )

    for j in range(GROUP):
        own_copy(j).wait()
    for index in range(GROUP):
        ring_copy(1, index).start()
        ring_copy(-1, index).start()
    for j in range(GROUP, BLOCKS):
        own_copy(j).wait()
    for index in range(GROUP, FLIGHT):
        ring_copy(1, index).start()
        ring_copy(-1, index).start()
    for j in range(BLOCKS):
        pair_copy(j, 0).start()

    forget_copy = pltpu.make_async_copy(forget_hbm, forget, forget_sem)
    forget_copy.start()
    gain_copy = pltpu.make_async_copy(gain_hbm, gain_ref, gain_sem)
    gain_copy.start()
    for r in ORDER:
        source = pl.ds(pl.multiple_of(lax.rem(y + 8 - r, 8) * 256, 256), 256)
        rows = pl.ds(PLACE[r] * 256, 256)
        for n, weight in enumerate((wk_hbm, wv_hbm, wq_hbm, wg_hbm)):
            pltpu.make_async_copy(weight.at[source], w.at[rows, pl.ds(n * 128, 128)], w_sem).start()

    forget_copy.wait()
    gain_copy.wait()
    v = jnp.exp2(jnp.full((16, 128), -exponent_ref[0].astype(F32)))
    series = jnp.full((16, 128), 1.0 / 8)
    for n in range(7, 0, -1):
        series = 1.0 / n + v * series
    logd = -v * series - forget[...]
    lane = lax.broadcasted_iota(jnp.int32, (16, 128), 1)
    row = lax.broadcasted_iota(jnp.int32, (16, 128), 0)
    run = logd
    for shift in (1, 2, 4, 8, 16, 32, 64):
        run = run + jnp.where(lane >= shift, pltpu.roll(run, shift, 1), 0.0)
    half_sum = jnp.broadcast_to(run[:, 127:128], (16, 128))
    run = run + jnp.where(row % 2 == 1, pltpu.roll(half_sum, 1, 0), 0.0)
    turned = run.T
    before = jnp.zeros((8, 128), F32)
    for j in range(BLOCKS):
        end = jnp.broadcast_to(run[2 * j + 1 : 2 * j + 2, 127:128], (8, 128))
        ends[0, j] = end
        ends[1, j] = before
        before = before + end
    own_total[...] = before

    def total_copy(e):
        return pltpu.make_async_remote_copy(
            src_ref=own_total, dst_ref=got_total.at[e - 1], send_sem=total_sent.at[e - 1],
            recv_sem=total_sem.at[e - 1], device_id={"seq": lax.rem(z + e, 8)}, device_id_type=MESH,
        )

    def state_copy(e):
        return pltpu.make_async_remote_copy(
            src_ref=own_state, dst_ref=got_state.at[e - 1], send_sem=state_sent.at[e - 1],
            recv_sem=state_sem.at[e - 1], device_id={"seq": lax.rem(z + e, 8)}, device_id_type=MESH,
        )

    def make_decay(j):
        rows = pl.ds(j * BLOCK, BLOCK)
        down = jnp.concatenate([turned[:, 2 * j : 2 * j + 1], turned[:, 2 * j + 1 : 2 * j + 2]], axis=0)
        across = jnp.concatenate([run[2 * j : 2 * j + 1], run[2 * j + 1 : 2 * j + 2]], axis=1)
        t = lax.broadcasted_iota(jnp.int32, (BLOCK, BLOCK), 0)
        s = lax.broadcasted_iota(jnp.int32, (BLOCK, BLOCK), 1)
        gap = jnp.where(t >= s, down - across, 0.0)
        decay[j] = jnp.where(t >= s, jnp.exp(gap), 0.0)
        wide = jnp.broadcast_to(down, (BLOCK, DH))
        qdec[rows] = jnp.exp(wide)
        kdec[rows] = jnp.exp(ends[0, j, 0:1] - wide)

    def wait_weights():
        pltpu.make_async_copy(w, w, w_sem).wait()

    def wait_pair(j, part):
        first, last = PLACES[part]
        spot = tok.at[pl.ds(j * BLOCK, BLOCK), pl.ds(0, 128 * (last - first))]
        pltpu.make_async_copy(spot, spot, pair_sem.at[j, part]).wait()

    def add_part(j, part):
        wait_pair(j, part)
        first, last = PLACES[part]
        span = pl.ds(first * 256, (last - first) * 256)
        rows = pl.ds(j * BLOCK, BLOCK)
        product = dot(tok[rows, span], w[span, :])
        if part:
            partial[rows] += product
        else:
            partial[rows] = product

    def finish_kv(rows, count):
        both = partial[rows, :256] + dot(tok[rows, 1792:2048], w[1792:2048, :256])
        keys = (both[:, :128] * DH**-0.5).astype(BF16)
        values = both[:, 128:].astype(BF16)
        kb[rows] = keys
        vb[rows] = values
        faded = (keys.astype(F32) * kdec[rows]).astype(BF16)
        return [
            t_dot(faded[n * BLOCK : (n + 1) * BLOCK], values[n * BLOCK : (n + 1) * BLOCK]) for n in range(count)
        ]

    def finish_qg(rows, block, count):
        both = partial[rows, 256:] + dot(tok[rows, 1792:2048], w[1792:2048, 256:])
        queries = both[:, :128].astype(BF16)
        gate = both[:, 128:].astype(BF16).astype(F32)
        sg[rows] = gate / (1.0 + jnp.exp(-gate)) * gain_ref[pl.ds(m, 1), :]
        qd[rows] = (queries.astype(F32) * qdec[rows]).astype(BF16)
        for n in range(count):
            span = pl.ds((block + n) * BLOCK, BLOCK)
            scores = (dot_t(queries[n * BLOCK : (n + 1) * BLOCK], kb[span]) * decay[block + n]).astype(BF16)
            olocal[span] = dot(scores, vb[span])

    def two(block):
        return pl.ds(block * BLOCK, 2 * BLOCK)

    def advance(block, added):
        state = carried[...]
        for n, more in enumerate(added):
            start[block + n] = state
            state = jnp.exp(ends[0, block + n, 0:1]) * state + more
        return state

    carried[...] = jnp.zeros_like(carried)
    for index in range(SENDS):
        for direction in (1, -1):
            ring_copy(direction, index).wait_recv()
            for later in range(FLIGHT, SENDS):
                if START[later] == index:
                    ring_copy(direction, later).start()
            j, d = (RIGHT if direction > 0 else LEFT)[index]
            pair_copy(j, d if direction > 0 else 8 - d).start()
        if index < BLOCKS:
            make_decay(index)
        if index == 3:
            wait_weights()
        if index == 14:
            for e in range(1, 8):

                @pl.when(z + e < 8)
                def _():
                    pl.semaphore_wait(later_in.at[e - 1], 1)
                    total_copy(e).start()

        if 4 <= index < 8:
            add_part(index - 4, 0)
        if index in (10, 11):
            add_part(2 * index - 20, 1)
            add_part(2 * index - 19, 1)
        if 12 <= index < 16:
            add_part(index - 8, 0)
        if index in (16, 17):
            add_part(2 * index - 32, 2)
            add_part(2 * index - 31, 2)
        if index in (20, 21):
            block = 2 * index - 40
            wait_pair(block, 3)
            wait_pair(block + 1, 3)
            carried[...] = advance(block, finish_kv(two(block), 2))
        if index in (22, 23):
            add_part(2 * index - 40, 1)
            add_part(2 * index - 39, 1)
        if index in (24, 25):
            finish_qg(two(2 * index - 48), 2 * index - 48, 2)
        if index == 26:
            for j in range(GROUP, BLOCKS):
                add_part(j, 2)

    for block in (GROUP, GROUP + 2):
        wait_pair(block, 3)
        wait_pair(block + 1, 3)
        carried[...] = advance(block, finish_kv(two(block), 2))
    own_state[...] = carried[...].astype(BF16)
    for e in range(7, 0, -1):

        @pl.when(z + e < 8)
        def _():
            state_copy(e).start()

    finish_qg(pl.ds(GROUP * BLOCK, GROUP * BLOCK), GROUP, GROUP)
    for j in range(BLOCKS):
        rows = pl.ds(j * BLOCK, BLOCK)
        olocal[rows] += dot(qd[rows], start[j].astype(BF16))

    carried[...] = jnp.zeros_like(carried)
    states[...] = jnp.zeros_like(states)
    for e in range(1, 8):

        @pl.when(z >= e)
        def _():
            total_copy(e).wait_recv()
            state_copy(e).wait_recv()
            carried[...] += jnp.exp(states[0:1]) * got_state[e - 1].astype(F32)
            states[...] += got_total[e - 1]

    entering = carried[...].astype(BF16)
    one = jnp.ones((8, 128), BF16)

    def out_copy(j, other, r):
        target = 2 * j + other
        return (
            pltpu.make_async_remote_copy(
                src_ref=ubuf.at[j, pl.ds(pl.multiple_of(other * 128, 128), 128)], dst_ref=out_ref.at[:, pl.ds(pl.multiple_of(m * 128, 128), 128)], send_sem=o_sent, recv_sem=o_sem,
                device_id={"mp": target}, device_id_type=MESH,
            ),
            pltpu.make_async_remote_copy(
                src_ref=ssbuf.at[j, other, pl.ds(0, 1)], dst_ref=ssgot.at[m, pl.ds(0, 1)], send_sem=ss_sent, recv_sem=ss_sem,
                device_id={"mp": target}, device_id_type=MESH,
            ),
        )

    for r in (4, 3, 5, 2, 6, 1, 7, 0):
        j = lax.rem(y + r, 8)
        rows = pl.ds(pl.multiple_of(j * BLOCK, BLOCK), BLOCK)
        o = (olocal[rows] + jnp.exp(ends[1, j, 0:1]) * dot(qd[rows], entering)).astype(BF16).astype(F32)
        ubuf[j] = (sg[rows] * o).astype(BF16)
        square = o * o
        high = square.astype(BF16)
        low = (square - high.astype(F32)).astype(BF16)
        total = dot_t(one, high) + dot_t(one, low)
        ssbuf[j, 0] = total[:, :128]
        ssbuf[j, 1] = total[:, 128:]
        if r:
            for other in (0, 1):
                for copy in out_copy(j, other, r):
                    copy.start()
        else:
            for copy in out_copy(j, 1 - core, r):
                copy.start()
            mine = pl.ds(pl.multiple_of(core * 128, 128), 128)
            keep = (
                pltpu.make_async_copy(ubuf.at[j, mine], out_ref.at[:, pl.ds(pl.multiple_of(m * 128, 128), 128)], self_sem.at[0]),
                pltpu.make_async_copy(ssbuf.at[j, core, pl.ds(0, 1)], ssgot.at[m, pl.ds(0, 1)], self_sem.at[1]),
            )
            for copy in keep:
                copy.start()
            for copy in keep:
                copy.wait()

    pltpu.make_async_copy(ssgot.at[pl.ds(0, 15), pl.ds(0, 1)], ssgot.at[pl.ds(0, 15), pl.ds(0, 1)], ss_sem).wait()
    pltpu.make_async_copy(out_ref.at[:, pl.ds(0, 1920)], out_ref.at[:, pl.ds(0, 1920)], o_sem).wait()
    squares = ssgot[0, 0:1]
    for n in range(1, 16):
        squares = squares + ssgot[n, 0:1]
    rstd = lax.rsqrt(squares / 2048.0 + 1e-06)
    down_ref[...] = jnp.broadcast_to(rstd, (128, 128)).T

    for sem in (sent_right, sent_left):
        spot = tok.at[pl.ds(0, SENDS * 16), :]
        pltpu.make_async_copy(spot, spot, sem).wait()
    spot = tok.at[:, pl.ds(0, 1024)]
    pltpu.make_async_copy(spot, spot, sent_pair).wait()
    pltpu.make_async_copy(out_ref.at[:, pl.ds(0, 1920)], out_ref.at[:, pl.ds(0, 1920)], o_sent).wait()
    pltpu.make_async_copy(ssgot.at[pl.ds(0, 15), pl.ds(0, 1)], ssgot.at[pl.ds(0, 15), pl.ds(0, 1)], ss_sent).wait()
    for e in range(1, 8):

        @pl.when(z + e < 8)
        def _():
            total_copy(e).wait_send()
            state_copy(e).wait_send()


def body(tokens, w_query, w_key, w_value, w_gate, decay_exponent, forget, norm_gain):
    gain = norm_gain.reshape(16, 128)
    vmem = pl.BlockSpec(memory_space=pltpu.VMEM)
    anywhere = pl.BlockSpec(memory_space=pl.ANY)
    dma = pltpu.SemaphoreType.DMA
    raw, down = pl.pallas_call(
        kernel,
        out_shape=(pltpu.VMEM((128, 2048), BF16), pltpu.VMEM((128, 128), F32)),
        in_specs=[anywhere] * 6 + [pl.BlockSpec(memory_space=pltpu.SMEM), anywhere],
        out_specs=(vmem, vmem),
        scratch_shapes=[
            pltpu.VMEM((2048, 2048), BF16),
            pltpu.VMEM((2048, 512), BF16),
            pltpu.VMEM((8, BLOCK, BLOCK), F32),
            pltpu.VMEM((2048, 128), F32),
            pltpu.VMEM((2048, 128), F32),
            pltpu.VMEM((2, 8, 8, 128), F32),
            pltpu.VMEM((2048, 128), F32),
            pltpu.VMEM((2048, 128), BF16),
            pltpu.VMEM((2048, 128), BF16),
            pltpu.VMEM((2048, 128), BF16),
            pltpu.VMEM((2048, 128), F32),
            pltpu.VMEM((8, 128), F32),
            pltpu.VMEM((8, 128, 128), F32),
            pltpu.VMEM((128, 128), BF16),
            pltpu.VMEM((8, 128), F32),
            pltpu.VMEM((7, 128, 128), BF16),
            pltpu.VMEM((7, 8, 128), F32),
            pltpu.VMEM((8, BLOCK, 128), BF16),
            pltpu.VMEM((8, 2, 8, 128), F32),
            pltpu.VMEM((16, 8, 128), F32),
            pltpu.VMEM((128, 128), F32),
            pltpu.VMEM((16, 128), F32),
            pltpu.VMEM((2048, 512), F32),
            pltpu.VMEM((16, 128), F32),
            dma((8,)), dma(()), dma((SENDS,)), dma((SENDS,)), dma((8, 4)), dma(()), dma(()), dma(()),
            dma((7,)), dma((7,)), dma((7,)), dma((7,)), dma(()), dma(()), dma(()), dma(()), dma((2,)),
            pltpu.SemaphoreType.REGULAR((7,)), dma(()), dma(()),
        ],
        compiler_params=pltpu.CompilerParams(
            collective_id=0, has_side_effects=True, vmem_limit_bytes=67043328 - 1100 * 1024
        ),
        name="retention_all",
    )(tokens, w_query, w_key, w_value, w_gate, forget.reshape(16, 128), decay_exponent, gain)
    return (raw.astype(F32) * down[:, :1]).astype(BF16)


def solution(mesh):
    placed = (
        P(("dp", "seq"), "mp"),
        P(None, "mp"),
        P(None, "mp"),
        P(None, "mp"),
        P(None, "mp"),
        P("mp"),
        P(("dp", "seq"), "mp"),
        P(),
    )
    return jax.shard_map(
        body, mesh=mesh, in_specs=placed, out_specs=P(("dp", "seq", "mp"), None), check_vma=False
    )
```

```python
import jax
import jax.numpy as jnp
from jax import lax
from jax.experimental import pallas as pl
from jax.experimental.pallas import tpu as pltpu
from jax.sharding import PartitionSpec as P

DH = 128
CHIPS = 8
BLOCK = 256
BLOCKS = 8
GROUP = 4
MESH = pl.DeviceIdType.MESH
F32 = jnp.float32
BF16 = jnp.bfloat16
PLACE = {0: 0, 1: 1, 7: 2, 2: 3, 6: 4, 3: 5, 5: 6, 4: 7}
ORDER = [0, 1, 7, 2, 6, 3, 5, 4]


def ring_lists():
    near, far = [0, 2, 1, 3], [4, 6, 5, 7]
    order = [(j, 1) for j in near] + [(j, 1) for j in far[:2]]
    order += [(j, 2) for j in near] + [(j, 1) for j in far[2:]]
    order += [(j, 3) for j in near] + [(j, 2) for j in far[:2]]
    order += [(j, 4) for j in near[:2]] + [(j, 2) for j in far[2:]]
    order += [(j, 3) for j in far] + [(j, 4) for j in far[:2]]
    return order, [(j + 1 - 2 * (j % 2), d) for j, d in order]


RIGHT, LEFT = ring_lists()
FLIGHT = 6
START = [max(n - FLIGHT, RIGHT.index((j, d - 1)) if d > 1 else -1) for n, (j, d) in enumerate(RIGHT)]
SENDS = len(RIGHT)
PART = {0: 0, 1: 0, 7: 0, 2: 1, 6: 1, 3: 2, 5: 2, 4: 3}
PLACES = ((0, 3), (3, 5), (5, 7), (7, 8))


def dot(a, b):
    return jnp.dot(a, b, preferred_element_type=F32)


def dot_t(a, b):
    return lax.dot_general(a, b, (((1,), (1,)), ((), ())), preferred_element_type=F32)


def t_dot(a, b):
    return lax.dot_general(a, b, (((0,), (0,)), ((), ())), preferred_element_type=F32)


def kernel(
    tok_hbm, wq_hbm, wk_hbm, wv_hbm, wg_hbm, forget_hbm, exponent_ref, gain_hbm, out_ref, down_ref,
    tok, w, decay, kdec, qdec, ends, sg, qd, vb, kb, olocal, states, start, own_state, own_total,
    got_state, got_total, ubuf, ssbuf, ssgot, carried, forget, partial, gain_ref, reach,
    tok_sem, w_sem, right_sem, left_sem, pair_sem, sent_right, sent_left, sent_pair,
    state_sem, total_sem, state_sent, total_sent, o_sem, ss_sem, o_sent, ss_sent, self_sem, later_in, forget_sem, gain_sem,
):
    m = lax.axis_index("mp")
    z = lax.axis_index("seq")
    core = lax.rem(m, 2)
    y = m // 2
    pair = m + 1 - 2 * core
    to_right = lax.rem(m + 2, 16)
    to_left = lax.rem(m + 14, 16)

    def columns(place, of):
        return pl.ds(pl.multiple_of(place * 256 + of * 128, 128), 128)

    def own_copy(j):
        rows = pl.ds(j * BLOCK, BLOCK)
        return pltpu.make_async_copy(tok_hbm.at[rows], tok.at[rows, columns(0, core)], tok_sem.at[j])

    for j in (0, 1, 2, 3, 4, 5, 6, 7):
        own_copy(j).start()

    barrier = pltpu.get_barrier_semaphore()
    for near in (to_left, to_right, pair):
        pl.semaphore_signal(barrier, inc=1, device_id={"mp": near}, device_id_type=MESH)
    for e in range(1, 8):

        @pl.when(z + e < 8)
        def _():
            pl.semaphore_signal(barrier, inc=1, device_id={"seq": lax.rem(z + e, 8)}, device_id_type=MESH)
    pl.semaphore_wait(barrier, 3 + z)
    for e in range(1, 8):

        @pl.when(z >= e)
        def _():
            pl.semaphore_signal(later_in.at[e - 1], inc=1, device_id={"seq": lax.rem(z + 8 - e, 8)}, device_id_type=MESH)


    def ring_copy(direction, index):
        j, d = (RIGHT if direction > 0 else LEFT)[index]
        source = (d - 1) if direction > 0 else (8 - (d - 1)) % 8
        target = d if direction > 0 else 8 - d
        rows = pl.ds(j * BLOCK, BLOCK)
        return pltpu.make_async_remote_copy(
            src_ref=tok.at[rows, columns(PLACE[source], core)],
            dst_ref=tok.at[rows, columns(PLACE[target], core)],
            send_sem=sent_right if direction > 0 else sent_left,
            recv_sem=(right_sem if direction > 0 else left_sem).at[index],
            device_id={"mp": to_right if direction > 0 else to_left},
            device_id_type=MESH,
        )

    def pair_copy(j, r):
        rows = pl.ds(j * BLOCK, BLOCK)
        spot = tok.at[rows, columns(PLACE[r], core)]
        return pltpu.make_async_remote_copy(
            src_ref=spot, dst_ref=spot, send_sem=sent_pair, recv_sem=pair_sem.at[j, PART[r]],
            device_id={"mp": pair}, device_id_type=MESH,
        )

    unloaded = [0, 1, 2, 3, 4, 5, 6, 7]
    for index in range(FLIGHT):
        for j in (RIGHT[index][0], LEFT[index][0]):
            if j in unloaded:
                own_copy(j).wait()
                unloaded.remove(j)
        ring_copy(1, index).start()
        ring_copy(-1, index).start()
    for j in unloaded:
        own_copy(j).wait()
    for j in range(BLOCKS):
        pair_copy(j, 0).start()

    forget_copy = pltpu.make_async_copy(forget_hbm, forget, forget_sem)
    forget_copy.start()
    gain_copy = pltpu.make_async_copy(gain_hbm, gain_ref, gain_sem)
    gain_copy.start()
    for r in ORDER:
        source = pl.ds(pl.multiple_of(lax.rem(y + 8 - r, 8) * 256, 256), 256)
        rows = pl.ds(PLACE[r] * 256, 256)
        for n, weight in enumerate((wk_hbm, wv_hbm, wq_hbm, wg_hbm)):
            pltpu.make_async_copy(weight.at[source], w.at[rows, pl.ds(n * 128, 128)], w_sem).start()

    forget_copy.wait()
    gain_copy.wait()
    v = jnp.exp2(jnp.full((16, 128), -exponent_ref[0].astype(F32)))
    series = jnp.full((16, 128), 1.0 / 8)
    for n in range(7, 0, -1):
        series = 1.0 / n + v * series
    logd = -v * series - forget[...]
    lane = lax.broadcasted_iota(jnp.int32, (16, 128), 1)
    row = lax.broadcasted_iota(jnp.int32, (16, 128), 0)
    run = logd
    for shift in (1, 2, 4, 8, 16, 32, 64):
        run = run + jnp.where(lane >= shift, pltpu.roll(run, shift, 1), 0.0)
    half_sum = jnp.broadcast_to(run[:, 127:128], (16, 128))
    run = run + jnp.where(row % 2 == 1, pltpu.roll(half_sum, 1, 0), 0.0)
    turned = run.T
    before = jnp.zeros((8, 128), F32)
    for j in range(BLOCKS):
        end = jnp.broadcast_to(run[2 * j + 1 : 2 * j + 2, 127:128], (8, 128))
        ends[0, j] = end
        ends[1, j] = before
        before = before + end
    own_total[...] = before

    def total_copy(e):
        return pltpu.make_async_remote_copy(
            src_ref=own_total, dst_ref=got_total.at[e - 1], send_sem=total_sent.at[e - 1],
            recv_sem=total_sem.at[e - 1], device_id={"seq": lax.rem(z + e, 8)}, device_id_type=MESH,
        )

    def state_copy(e):
        return pltpu.make_async_remote_copy(
            src_ref=own_state, dst_ref=got_state.at[e - 1], send_sem=state_sent.at[e - 1],
            recv_sem=state_sem.at[e - 1], device_id={"seq": lax.rem(z + e, 8)}, device_id_type=MESH,
        )

    def make_decay(j):
        rows = pl.ds(j * BLOCK, BLOCK)
        down = jnp.concatenate([turned[:, 2 * j : 2 * j + 1], turned[:, 2 * j + 1 : 2 * j + 2]], axis=0)
        across = jnp.concatenate([run[2 * j : 2 * j + 1], run[2 * j + 1 : 2 * j + 2]], axis=1)
        t = lax.broadcasted_iota(jnp.int32, (BLOCK, BLOCK), 0)
        s = lax.broadcasted_iota(jnp.int32, (BLOCK, BLOCK), 1)
        gap = jnp.where(t >= s, down - across, 0.0)
        decay[j] = jnp.where(t >= s, jnp.exp(gap), 0.0)
        wide = jnp.broadcast_to(down, (BLOCK, DH))
        qdec[rows] = jnp.exp(wide)
        kdec[rows] = jnp.exp(ends[0, j, 0:1] - wide)

    def wait_weights():
        pltpu.make_async_copy(w, w, w_sem).wait()

    def wait_pair(j, part):
        first, last = PLACES[part]
        spot = tok.at[pl.ds(j * BLOCK, BLOCK), pl.ds(0, 128 * (last - first))]
        pltpu.make_async_copy(spot, spot, pair_sem.at[j, part]).wait()

    def add_part(j, part):
        wait_pair(j, part)
        first, last = PLACES[part]
        span = pl.ds(first * 256, (last - first) * 256)
        rows = pl.ds(j * BLOCK, BLOCK)
        product = dot(tok[rows, span], w[span, :])
        if part:
            partial[rows] += product
        else:
            partial[rows] = product

    def finish_kv(rows, count):
        both = partial[rows, :256] + dot(tok[rows, 1792:2048], w[1792:2048, :256])
        keys = (both[:, :128] * DH**-0.5).astype(BF16)
        values = both[:, 128:].astype(BF16)
        kb[rows] = keys
        vb[rows] = values
        faded = (keys.astype(F32) * kdec[rows]).astype(BF16)
        return [
            t_dot(faded[n * BLOCK : (n + 1) * BLOCK], values[n * BLOCK : (n + 1) * BLOCK]) for n in range(count)
        ]

    def finish_qg(rows, block, count):
        both = partial[rows, 256:] + dot(tok[rows, 1792:2048], w[1792:2048, 256:])
        queries = both[:, :128].astype(BF16)
        gate = both[:, 128:].astype(BF16).astype(F32)
        sg[rows] = gate / (1.0 + jnp.exp(-gate)) * gain_ref[pl.ds(m, 1), :]
        qd[rows] = (queries.astype(F32) * qdec[rows]).astype(BF16)
        for n in range(count):
            span = pl.ds((block + n) * BLOCK, BLOCK)
            scores = (dot_t(queries[n * BLOCK : (n + 1) * BLOCK], kb[span]) * decay[block + n]).astype(BF16)
            olocal[span] = dot(scores, vb[span])

    def add_local(lower, upper):
        for j in range(lower, upper):
            rows = pl.ds(j * BLOCK, BLOCK)
            olocal[rows] += dot(qd[rows], start[j].astype(BF16))

    def two(block):
        return pl.ds(block * BLOCK, 2 * BLOCK)

    def advance(block, added):
        state = carried[...]
        for n, more in enumerate(added):
            start[block + n] = state
            state = jnp.exp(ends[0, block + n, 0:1]) * state + more
        return state

    carried[...] = jnp.zeros_like(carried)
    for index in range(SENDS):
        for direction in (1, -1):
            ring_copy(direction, index).wait_recv()
            for later in range(FLIGHT, SENDS):
                if START[later] == index:
                    ring_copy(direction, later).start()
            j, d = (RIGHT if direction > 0 else LEFT)[index]
            pair_copy(j, d if direction > 0 else 8 - d).start()
        if index < BLOCKS:
            make_decay(index)
        if index == 3:
            wait_weights()
        if index == 14:
            for e in range(1, 8):

                @pl.when(z + e < 8)
                def _():
                    pl.semaphore_wait(later_in.at[e - 1], 1)
                    total_copy(e).start()

        if index == 23:
            states[...] = jnp.zeros_like(states)
            for e in range(1, 8):

                @pl.when(z >= e)
                def _():
                    total_copy(e).wait_recv()
                    reach[e - 1] = jnp.exp(states[...])
                    states[...] += got_total[e - 1]

        if 4 <= index < 8:
            add_part(index - 4, 0)
        if index in (10, 11):
            add_part(2 * index - 20, 1)
            add_part(2 * index - 19, 1)
        if 12 <= index < 16:
            add_part(index - 8, 0)
        if index in (16, 17):
            add_part(2 * index - 32, 2)
            add_part(2 * index - 31, 2)
        if index in (20, 21):
            block = 2 * index - 40
            wait_pair(block, 3)
            wait_pair(block + 1, 3)
            carried[...] = advance(block, finish_kv(two(block), 2))
        if index in (22, 23):
            add_part(2 * index - 40, 1)
            add_part(2 * index - 39, 1)
        if index in (24, 25):
            finish_qg(two(2 * index - 48), 2 * index - 48, 2)
        if index == 26:
            for j in range(GROUP, BLOCKS):
                add_part(j, 2)

    add_local(0, GROUP)

    for block in (GROUP, GROUP + 2):
        wait_pair(block, 3)
        wait_pair(block + 1, 3)
        carried[...] = advance(block, finish_kv(two(block), 2))
    own_state[...] = carried[...].astype(BF16)
    for e in range(7, 0, -1):

        @pl.when(z + e < 8)
        def _():
            state_copy(e).start()

    finish_qg(pl.ds(GROUP * BLOCK, GROUP * BLOCK), GROUP, GROUP)
    add_local(GROUP, BLOCKS)

    carried[...] = jnp.zeros_like(carried)
    for e in range(1, 8):

        @pl.when(z >= e)
        def _():
            state_copy(e).wait_recv()
            carried[...] += reach[e - 1, 0:1] * got_state[e - 1].astype(F32)

    entering = carried[...].astype(BF16)
    one = jnp.ones((8, 128), BF16)

    def out_copy(j, other, r):
        target = 2 * j + other
        return (
            pltpu.make_async_remote_copy(
                src_ref=ubuf.at[j, pl.ds(pl.multiple_of(other * 128, 128), 128)], dst_ref=out_ref.at[:, pl.ds(pl.multiple_of(m * 128, 128), 128)], send_sem=o_sent, recv_sem=o_sem,
                device_id={"mp": target}, device_id_type=MESH,
            ),
            pltpu.make_async_remote_copy(
                src_ref=ssbuf.at[j, other, pl.ds(0, 1)], dst_ref=ssgot.at[m, pl.ds(0, 1)], send_sem=ss_sent, recv_sem=ss_sem,
                device_id={"mp": target}, device_id_type=MESH,
            ),
        )

    for r in (4, 3, 5, 2, 6, 1, 7, 0):
        j = lax.rem(y + r, 8)
        for part in ((0, 1), (1, 1)) if r == 4 else ((0, 2),):
            rows = pl.ds(pl.multiple_of(j * BLOCK + part[0] * 128, 128), part[1] * 128)
            o = (olocal[rows] + jnp.exp(ends[1, j, 0:1]) * dot(qd[rows], entering)).astype(BF16).astype(F32)
            ubuf[j, pl.ds(part[0] * 128, part[1] * 128)] = (sg[rows] * o).astype(BF16)
            square = o * o
            high = square.astype(BF16)
            low = (square - high.astype(F32)).astype(BF16)
            total = dot_t(one, high) + dot_t(one, low)
            for n in range(part[1]):
                ssbuf[j, part[0] + n] = total[:, n * 128 : (n + 1) * 128]
            if r == 4:
                for copy in out_copy(j, part[0], r):
                    copy.start()
        if r == 4:
            pass
        elif r:
            for other in (0, 1):
                for copy in out_copy(j, other, r):
                    copy.start()
        else:
            for copy in out_copy(j, 1 - core, r):
                copy.start()
            mine = pl.ds(pl.multiple_of(core * 128, 128), 128)
            keep = (
                pltpu.make_async_copy(ubuf.at[j, mine], out_ref.at[:, pl.ds(pl.multiple_of(m * 128, 128), 128)], self_sem.at[0]),
                pltpu.make_async_copy(ssbuf.at[j, core, pl.ds(0, 1)], ssgot.at[m, pl.ds(0, 1)], self_sem.at[1]),
            )
            for copy in keep:
                copy.start()
            for copy in keep:
                copy.wait()

    pltpu.make_async_copy(ssgot.at[pl.ds(0, 15), pl.ds(0, 1)], ssgot.at[pl.ds(0, 15), pl.ds(0, 1)], ss_sem).wait()
    pltpu.make_async_copy(out_ref.at[:, pl.ds(0, 1920)], out_ref.at[:, pl.ds(0, 1920)], o_sem).wait()
    squares = ssgot[0, 0:1]
    for n in range(1, 16):
        squares = squares + ssgot[n, 0:1]
    rstd = lax.rsqrt(squares / 2048.0 + 1e-06)
    down_ref[...] = jnp.broadcast_to(rstd, (128, 128)).T

    for sem in (sent_right, sent_left):
        spot = tok.at[pl.ds(0, SENDS * 16), :]
        pltpu.make_async_copy(spot, spot, sem).wait()
    spot = tok.at[:, pl.ds(0, 1024)]
    pltpu.make_async_copy(spot, spot, sent_pair).wait()
    pltpu.make_async_copy(out_ref.at[:, pl.ds(0, 1920)], out_ref.at[:, pl.ds(0, 1920)], o_sent).wait()
    pltpu.make_async_copy(ssgot.at[pl.ds(0, 15), pl.ds(0, 1)], ssgot.at[pl.ds(0, 15), pl.ds(0, 1)], ss_sent).wait()
    for e in range(1, 8):

        @pl.when(z + e < 8)
        def _():
            total_copy(e).wait_send()
            state_copy(e).wait_send()


def body(tokens, w_query, w_key, w_value, w_gate, decay_exponent, forget, norm_gain):
    gain = norm_gain.reshape(16, 128)
    vmem = pl.BlockSpec(memory_space=pltpu.VMEM)
    anywhere = pl.BlockSpec(memory_space=pl.ANY)
    dma = pltpu.SemaphoreType.DMA
    raw, down = pl.pallas_call(
        kernel,
        out_shape=(pltpu.VMEM((128, 2048), BF16), pltpu.VMEM((128, 128), F32)),
        in_specs=[anywhere] * 6 + [pl.BlockSpec(memory_space=pltpu.SMEM), anywhere],
        out_specs=(vmem, vmem),
        scratch_shapes=[
            pltpu.VMEM((2048, 2048), BF16),
            pltpu.VMEM((2048, 512), BF16),
            pltpu.VMEM((8, BLOCK, BLOCK), F32),
            pltpu.VMEM((2048, 128), F32),
            pltpu.VMEM((2048, 128), F32),
            pltpu.VMEM((2, 8, 8, 128), F32),
            pltpu.VMEM((2048, 128), F32),
            pltpu.VMEM((2048, 128), BF16),
            pltpu.VMEM((2048, 128), BF16),
            pltpu.VMEM((2048, 128), BF16),
            pltpu.VMEM((2048, 128), F32),
            pltpu.VMEM((8, 128), F32),
            pltpu.VMEM((8, 128, 128), F32),
            pltpu.VMEM((128, 128), BF16),
            pltpu.VMEM((8, 128), F32),
            pltpu.VMEM((7, 128, 128), BF16),
            pltpu.VMEM((7, 8, 128), F32),
            pltpu.VMEM((8, BLOCK, 128), BF16),
            pltpu.VMEM((8, 2, 8, 128), F32),
            pltpu.VMEM((16, 8, 128), F32),
            pltpu.VMEM((128, 128), F32),
            pltpu.VMEM((16, 128), F32),
            pltpu.VMEM((2048, 512), F32),
            pltpu.VMEM((16, 128), F32),
            pltpu.VMEM((7, 8, 128), F32),
            dma((8,)), dma(()), dma((SENDS,)), dma((SENDS,)), dma((8, 4)), dma(()), dma(()), dma(()),
            dma((7,)), dma((7,)), dma((7,)), dma((7,)), dma(()), dma(()), dma(()), dma(()), dma((2,)),
            pltpu.SemaphoreType.REGULAR((7,)), dma(()), dma(()),
        ],
        compiler_params=pltpu.CompilerParams(
            collective_id=0, has_side_effects=True, vmem_limit_bytes=67043328 - 1100 * 1024
        ),
        name="retention_all",
    )(tokens, w_query, w_key, w_value, w_gate, forget.reshape(16, 128), decay_exponent, gain)
    return (raw.astype(F32) * down[:, :1]).astype(BF16)


def solution(mesh):
    placed = (
        P(("dp", "seq"), "mp"),
        P(None, "mp"),
        P(None, "mp"),
        P(None, "mp"),
        P(None, "mp"),
        P("mp"),
        P(("dp", "seq"), "mp"),
        P(),
    )
    return jax.shard_map(
        body, mesh=mesh, in_specs=placed, out_specs=P(("dp", "seq", "mp"), None), check_vma=False
    )
```

```python
import jax
import jax.numpy as jnp
from jax import lax
from jax.experimental import pallas as pl
from jax.experimental.pallas import tpu as pltpu
from jax.sharding import PartitionSpec as P

DH = 128
CHIPS = 8
BLOCK = 256
BLOCKS = 8
GROUP = 4
MESH = pl.DeviceIdType.MESH
F32 = jnp.float32
BF16 = jnp.bfloat16
PLACE = {0: 0, 1: 1, 7: 2, 2: 3, 6: 4, 3: 5, 5: 6, 4: 7}
ORDER = [0, 1, 7, 2, 6, 3, 5, 4]


def ring_lists():
    near, far = [0, 2, 1, 3], [4, 6, 5, 7]
    order = [(j, 1) for j in near] + [(j, 1) for j in far[:2]]
    order += [(j, 2) for j in near] + [(j, 1) for j in far[2:]]
    order += [(j, 3) for j in near] + [(j, 2) for j in far[:2]]
    order += [(j, 4) for j in near[:2]] + [(j, 2) for j in far[2:]]
    order += [(j, 3) for j in far] + [(j, 4) for j in far[:2]]
    return order, [(j + 1 - 2 * (j % 2), d) for j, d in order]


RIGHT, LEFT = ring_lists()
FLIGHT = 6
START = [max(n - FLIGHT, RIGHT.index((j, d - 1)) if d > 1 else -1) for n, (j, d) in enumerate(RIGHT)]
SENDS = len(RIGHT)
PART = {0: 0, 1: 0, 7: 0, 2: 1, 6: 1, 3: 2, 5: 2, 4: 3}
PLACES = ((0, 3), (3, 5), (5, 7), (7, 8))


def dot(a, b):
    return jnp.dot(a, b, preferred_element_type=F32)


def dot_t(a, b):
    return lax.dot_general(a, b, (((1,), (1,)), ((), ())), preferred_element_type=F32)


def t_dot(a, b):
    return lax.dot_general(a, b, (((0,), (0,)), ((), ())), preferred_element_type=F32)


def kernel(
    tok_hbm, wq_hbm, wk_hbm, wv_hbm, wg_hbm, forget_hbm, exponent_ref, gain_hbm, out_ref, down_ref,
    tok, w, decay, kdec, qdec, ends, sg, qd, vb, kb, olocal, states, start, own_state, own_total,
    got_state, got_total, ubuf, ssbuf, ssgot, carried, forget, partial, gain_ref,
    tok_sem, w_sem, right_sem, left_sem, pair_sem, sent_right, sent_left, sent_pair,
    state_sem, total_sem, state_sent, total_sent, o_sem, ss_sem, o_sent, ss_sent, self_sem, later_in, forget_sem, gain_sem,
):
    m = lax.axis_index("mp")
    z = lax.axis_index("seq")
    core = lax.rem(m, 2)
    y = m // 2
    pair = m + 1 - 2 * core
    to_right = lax.rem(m + 2, 16)
    to_left = lax.rem(m + 14, 16)

    def columns(place, of):
        return pl.ds(pl.multiple_of(place * 256 + of * 128, 128), 128)

    def own_copy(j):
        rows = pl.ds(j * BLOCK, BLOCK)
        return pltpu.make_async_copy(tok_hbm.at[rows], tok.at[rows, columns(0, core)], tok_sem.at[j])

    for j in (0, 2, 1, 3, 4, 6, 5, 7):
        own_copy(j).start()

    barrier = pltpu.get_barrier_semaphore()
    for near in (to_left, to_right, pair):
        pl.semaphore_signal(barrier, inc=1, device_id={"mp": near}, device_id_type=MESH)
    for e in range(1, 8):

        @pl.when(z + e < 8)
        def _():
            pl.semaphore_signal(barrier, inc=1, device_id={"seq": lax.rem(z + e, 8)}, device_id_type=MESH)
    pl.semaphore_wait(barrier, 3 + z)
    for e in range(1, 8):

        @pl.when(z >= e)
        def _():
            pl.semaphore_signal(later_in.at[e - 1], inc=1, device_id={"seq": lax.rem(z + 8 - e, 8)}, device_id_type=MESH)


    def ring_copy(direction, index):
        j, d = (RIGHT if direction > 0 else LEFT)[index]
        source = (d - 1) if direction > 0 else (8 - (d - 1)) % 8
        target = d if direction > 0 else 8 - d
        rows = pl.ds(j * BLOCK, BLOCK)
        return pltpu.make_async_remote_copy(
            src_ref=tok.at[rows, columns(PLACE[source], core)],
            dst_ref=tok.at[rows, columns(PLACE[target], core)],
            send_sem=sent_right if direction > 0 else sent_left,
            recv_sem=(right_sem if direction > 0 else left_sem).at[index],
            device_id={"mp": to_right if direction > 0 else to_left},
            device_id_type=MESH,
        )

    def pair_copy(j, r):
        rows = pl.ds(j * BLOCK, BLOCK)
        spot = tok.at[rows, columns(PLACE[r], core)]
        return pltpu.make_async_remote_copy(
            src_ref=spot, dst_ref=spot, send_sem=sent_pair, recv_sem=pair_sem.at[j, PART[r]],
            device_id={"mp": pair}, device_id_type=MESH,
        )

    for j in range(GROUP):
        own_copy(j).wait()
    for index in range(GROUP):
        ring_copy(1, index).start()
        ring_copy(-1, index).start()
    for j in range(GROUP, BLOCKS):
        own_copy(j).wait()
    for index in range(GROUP, FLIGHT):
        ring_copy(1, index).start()
        ring_copy(-1, index).start()
    for j in range(BLOCKS):
        pair_copy(j, 0).start()

    forget_copy = pltpu.make_async_copy(forget_hbm, forget, forget_sem)
    forget_copy.start()
    gain_copy = pltpu.make_async_copy(gain_hbm, gain_ref, gain_sem)
    gain_copy.start()
    for r in ORDER:
        source = pl.ds(pl.multiple_of(lax.rem(y + 8 - r, 8) * 256, 256), 256)
        rows = pl.ds(PLACE[r] * 256, 256)
        for n, weight in enumerate((wk_hbm, wv_hbm, wq_hbm, wg_hbm)):
            pltpu.make_async_copy(weight.at[source], w.at[rows, pl.ds(n * 128, 128)], w_sem).start()

    forget_copy.wait()
    gain_copy.wait()
    v = jnp.exp2(jnp.full((16, 128), -exponent_ref[0].astype(F32)))
    series = jnp.full((16, 128), 1.0 / 8)
    for n in range(7, 0, -1):
        series = 1.0 / n + v * series
    logd = -v * series - forget[...]
    lane = lax.broadcasted_iota(jnp.int32, (16, 128), 1)
    row = lax.broadcasted_iota(jnp.int32, (16, 128), 0)
    run = logd
    for shift in (1, 2, 4, 8, 16, 32, 64):
        run = run + jnp.where(lane >= shift, pltpu.roll(run, shift, 1), 0.0)
    half_sum = jnp.broadcast_to(run[:, 127:128], (16, 128))
    run = run + jnp.where(row % 2 == 1, pltpu.roll(half_sum, 1, 0), 0.0)
    turned = run.T
    before = jnp.zeros((8, 128), F32)
    for j in range(BLOCKS):
        end = jnp.broadcast_to(run[2 * j + 1 : 2 * j + 2, 127:128], (8, 128))
        ends[0, j] = end
        ends[1, j] = before
        before = before + end
    own_total[...] = before

    def total_copy(e):
        return pltpu.make_async_remote_copy(
            src_ref=own_total, dst_ref=got_total.at[e - 1], send_sem=total_sent.at[e - 1],
            recv_sem=total_sem.at[e - 1], device_id={"seq": lax.rem(z + e, 8)}, device_id_type=MESH,
        )

    def state_copy(e):
        return pltpu.make_async_remote_copy(
            src_ref=own_state, dst_ref=got_state.at[e - 1], send_sem=state_sent.at[e - 1],
            recv_sem=state_sem.at[e - 1], device_id={"seq": lax.rem(z + e, 8)}, device_id_type=MESH,
        )

    def make_decay(j):
        rows = pl.ds(j * BLOCK, BLOCK)
        down = jnp.concatenate([turned[:, 2 * j : 2 * j + 1], turned[:, 2 * j + 1 : 2 * j + 2]], axis=0)
        across = jnp.concatenate([run[2 * j : 2 * j + 1], run[2 * j + 1 : 2 * j + 2]], axis=1)
        t = lax.broadcasted_iota(jnp.int32, (BLOCK, BLOCK), 0)
        s = lax.broadcasted_iota(jnp.int32, (BLOCK, BLOCK), 1)
        gap = jnp.where(t >= s, down - across, 0.0)
        decay[j] = jnp.where(t >= s, jnp.exp(gap), 0.0)
        wide = jnp.broadcast_to(down, (BLOCK, DH))
        qdec[rows] = jnp.exp(wide)
        kdec[rows] = jnp.exp(ends[0, j, 0:1] - wide)

    def wait_weights():
        pltpu.make_async_copy(w, w, w_sem).wait()

    def wait_pair(j, part):
        first, last = PLACES[part]
        spot = tok.at[pl.ds(j * BLOCK, BLOCK), pl.ds(0, 128 * (last - first))]
        pltpu.make_async_copy(spot, spot, pair_sem.at[j, part]).wait()

    def add_part(j, part):
        wait_pair(j, part)
        first, last = PLACES[part]
        span = pl.ds(first * 256, (last - first) * 256)
        rows = pl.ds(j * BLOCK, BLOCK)
        product = dot(tok[rows, span], w[span, :])
        if part:
            partial[rows] += product
        else:
            partial[rows] = product

    def finish_kv(rows, count):
        both = partial[rows, :256] + dot(tok[rows, 1792:2048], w[1792:2048, :256])
        keys = (both[:, :128] * DH**-0.5).astype(BF16)
        values = both[:, 128:].astype(BF16)
        kb[rows] = keys
        vb[rows] = values
        faded = (keys.astype(F32) * kdec[rows]).astype(BF16)
        return [
            t_dot(faded[n * BLOCK : (n + 1) * BLOCK], values[n * BLOCK : (n + 1) * BLOCK]) for n in range(count)
        ]

    def finish_qg(rows, block, count):
        both = partial[rows, 256:] + dot(tok[rows, 1792:2048], w[1792:2048, 256:])
        queries = both[:, :128].astype(BF16)
        gate = both[:, 128:].astype(BF16).astype(F32)
        sg[rows] = gate / (1.0 + jnp.exp(-gate)) * gain_ref[pl.ds(m, 1), :]
        qd[rows] = (queries.astype(F32) * qdec[rows]).astype(BF16)
        for n in range(count):
            span = pl.ds((block + n) * BLOCK, BLOCK)
            scores = (dot_t(queries[n * BLOCK : (n + 1) * BLOCK], kb[span]) * decay[block + n]).astype(BF16)
            olocal[span] = dot(scores, vb[span])

    def add_local(lower, upper):
        for j in range(lower, upper):
            rows = pl.ds(j * BLOCK, BLOCK)
            olocal[rows] += dot(qd[rows], start[j].astype(BF16))

    def two(block):
        return pl.ds(block * BLOCK, 2 * BLOCK)

    def advance(block, added):
        state = carried[...]
        for n, more in enumerate(added):
            start[block + n] = state
            state = jnp.exp(ends[0, block + n, 0:1]) * state + more
        return state

    carried[...] = jnp.zeros_like(carried)
    for index in range(SENDS):
        for direction in (1, -1):
            ring_copy(direction, index).wait_recv()
            for later in range(FLIGHT, SENDS):
                if START[later] == index:
                    ring_copy(direction, later).start()
            j, d = (RIGHT if direction > 0 else LEFT)[index]
            pair_copy(j, d if direction > 0 else 8 - d).start()
        if index < BLOCKS:
            make_decay(index)
        if index == 3:
            wait_weights()
        if index == 14:
            for e in range(1, 8):

                @pl.when(z + e < 8)
                def _():
                    pl.semaphore_wait(later_in.at[e - 1], 1)
                    total_copy(e).start()

        if 4 <= index < 8:
            add_part(index - 4, 0)
        if index in (10, 11):
            add_part(2 * index - 20, 1)
            add_part(2 * index - 19, 1)
        if 12 <= index < 16:
            add_part(index - 8, 0)
        if index in (16, 17):
            add_part(2 * index - 32, 2)
            add_part(2 * index - 31, 2)
        if index in (20, 21):
            block = 2 * index - 40
            wait_pair(block, 3)
            wait_pair(block + 1, 3)
            carried[...] = advance(block, finish_kv(two(block), 2))
        if index in (22, 23):
            add_part(2 * index - 40, 1)
            add_part(2 * index - 39, 1)
        if index in (24, 25):
            finish_qg(two(2 * index - 48), 2 * index - 48, 2)
            add_local(2 * index - 48, 2 * index - 46)
        if index == 26:
            for j in range(GROUP, BLOCKS):
                add_part(j, 2)

    for block in (GROUP, GROUP + 2):
        wait_pair(block, 3)
        wait_pair(block + 1, 3)
        carried[...] = advance(block, finish_kv(two(block), 2))
    own_state[...] = carried[...].astype(BF16)
    for e in range(7, 0, -1):

        @pl.when(z + e < 8)
        def _():
            state_copy(e).start()

    finish_qg(pl.ds(GROUP * BLOCK, GROUP * BLOCK), GROUP, GROUP)
    add_local(GROUP, BLOCKS)

    carried[...] = jnp.zeros_like(carried)
    states[...] = jnp.zeros_like(states)
    for e in range(1, 8):

        @pl.when(z >= e)
        def _():
            total_copy(e).wait_recv()
            state_copy(e).wait_recv()
            carried[...] += jnp.exp(states[0:1]) * got_state[e - 1].astype(F32)
            states[...] += got_total[e - 1]

    entering = carried[...].astype(BF16)
    one = jnp.ones((8, 128), BF16)

    def out_copy(j, other, r):
        target = 2 * j + other
        return (
            pltpu.make_async_remote_copy(
                src_ref=ubuf.at[j, pl.ds(pl.multiple_of(other * 128, 128), 128)], dst_ref=out_ref.at[:, pl.ds(pl.multiple_of(m * 128, 128), 128)], send_sem=o_sent, recv_sem=o_sem,
                device_id={"mp": target}, device_id_type=MESH,
            ),
            pltpu.make_async_remote_copy(
                src_ref=ssbuf.at[j, other, pl.ds(0, 1)], dst_ref=ssgot.at[m, pl.ds(0, 1)], send_sem=ss_sent, recv_sem=ss_sem,
                device_id={"mp": target}, device_id_type=MESH,
            ),
        )

    for r in (4, 3, 5, 2, 6, 1, 7, 0):
        j = lax.rem(y + r, 8)
        rows = pl.ds(pl.multiple_of(j * BLOCK, BLOCK), BLOCK)
        o = (olocal[rows] + jnp.exp(ends[1, j, 0:1]) * dot(qd[rows], entering)).astype(BF16).astype(F32)
        ubuf[j] = (sg[rows] * o).astype(BF16)
        square = o * o
        high = square.astype(BF16)
        low = (square - high.astype(F32)).astype(BF16)
        total = dot_t(one, high) + dot_t(one, low)
        ssbuf[j, 0] = total[:, :128]
        ssbuf[j, 1] = total[:, 128:]
        if r:
            for other in (0, 1):
                for copy in out_copy(j, other, r):
                    copy.start()
        else:
            for copy in out_copy(j, 1 - core, r):
                copy.start()
            mine = pl.ds(pl.multiple_of(core * 128, 128), 128)
            keep = (
                pltpu.make_async_copy(ubuf.at[j, mine], out_ref.at[:, pl.ds(pl.multiple_of(m * 128, 128), 128)], self_sem.at[0]),
                pltpu.make_async_copy(ssbuf.at[j, core, pl.ds(0, 1)], ssgot.at[m, pl.ds(0, 1)], self_sem.at[1]),
            )
            for copy in keep:
                copy.start()
            for copy in keep:
                copy.wait()

    pltpu.make_async_copy(ssgot.at[pl.ds(0, 15), pl.ds(0, 1)], ssgot.at[pl.ds(0, 15), pl.ds(0, 1)], ss_sem).wait()
    pltpu.make_async_copy(out_ref.at[:, pl.ds(0, 1920)], out_ref.at[:, pl.ds(0, 1920)], o_sem).wait()
    squares = ssgot[0, 0:1]
    for n in range(1, 16):
        squares = squares + ssgot[n, 0:1]
    rstd = lax.rsqrt(squares / 2048.0 + 1e-06)
    down_ref[...] = jnp.broadcast_to(rstd, (128, 128)).T

    for sem in (sent_right, sent_left):
        spot = tok.at[pl.ds(0, SENDS * 16), :]
        pltpu.make_async_copy(spot, spot, sem).wait()
    spot = tok.at[:, pl.ds(0, 1024)]
    pltpu.make_async_copy(spot, spot, sent_pair).wait()
    pltpu.make_async_copy(out_ref.at[:, pl.ds(0, 1920)], out_ref.at[:, pl.ds(0, 1920)], o_sent).wait()
    pltpu.make_async_copy(ssgot.at[pl.ds(0, 15), pl.ds(0, 1)], ssgot.at[pl.ds(0, 15), pl.ds(0, 1)], ss_sent).wait()
    for e in range(1, 8):

        @pl.when(z + e < 8)
        def _():
            total_copy(e).wait_send()
            state_copy(e).wait_send()


def body(tokens, w_query, w_key, w_value, w_gate, decay_exponent, forget, norm_gain):
    gain = norm_gain.reshape(16, 128)
    vmem = pl.BlockSpec(memory_space=pltpu.VMEM)
    anywhere = pl.BlockSpec(memory_space=pl.ANY)
    dma = pltpu.SemaphoreType.DMA
    raw, down = pl.pallas_call(
        kernel,
        out_shape=(pltpu.VMEM((128, 2048), BF16), pltpu.VMEM((128, 128), F32)),
        in_specs=[anywhere] * 6 + [pl.BlockSpec(memory_space=pltpu.SMEM), anywhere],
        out_specs=(vmem, vmem),
        scratch_shapes=[
            pltpu.VMEM((2048, 2048), BF16),
            pltpu.VMEM((2048, 512), BF16),
            pltpu.VMEM((8, BLOCK, BLOCK), F32),
            pltpu.VMEM((2048, 128), F32),
            pltpu.VMEM((2048, 128), F32),
            pltpu.VMEM((2, 8, 8, 128), F32),
            pltpu.VMEM((2048, 128), F32),
            pltpu.VMEM((2048, 128), BF16),
            pltpu.VMEM((2048, 128), BF16),
            pltpu.VMEM((2048, 128), BF16),
            pltpu.VMEM((2048, 128), F32),
            pltpu.VMEM((8, 128), F32),
            pltpu.VMEM((8, 128, 128), F32),
            pltpu.VMEM((128, 128), BF16),
            pltpu.VMEM((8, 128), F32),
            pltpu.VMEM((7, 128, 128), BF16),
            pltpu.VMEM((7, 8, 128), F32),
            pltpu.VMEM((8, BLOCK, 128), BF16),
            pltpu.VMEM((8, 2, 8, 128), F32),
            pltpu.VMEM((16, 8, 128), F32),
            pltpu.VMEM((128, 128), F32),
            pltpu.VMEM((16, 128), F32),
            pltpu.VMEM((2048, 512), F32),
            pltpu.VMEM((16, 128), F32),
            dma((8,)), dma(()), dma((SENDS,)), dma((SENDS,)), dma((8, 4)), dma(()), dma(()), dma(()),
            dma((7,)), dma((7,)), dma((7,)), dma((7,)), dma(()), dma(()), dma(()), dma(()), dma((2,)),
            pltpu.SemaphoreType.REGULAR((7,)), dma(()), dma(()),
        ],
        compiler_params=pltpu.CompilerParams(
            collective_id=0, has_side_effects=True, vmem_limit_bytes=67043328 - 1100 * 1024
        ),
        name="retention_all",
    )(tokens, w_query, w_key, w_value, w_gate, forget.reshape(16, 128), decay_exponent, gain)
    return (raw.astype(F32) * down[:, :1]).astype(BF16)


def solution(mesh):
    placed = (
        P(("dp", "seq"), "mp"),
        P(None, "mp"),
        P(None, "mp"),
        P(None, "mp"),
        P(None, "mp"),
        P("mp"),
        P(("dp", "seq"), "mp"),
        P(),
    )
    return jax.shard_map(
        body, mesh=mesh, in_specs=placed, out_specs=P(("dp", "seq", "mp"), None), check_vma=False
    )
```
